256 devices in a mesh: nodes: 64 (over z, y, core), rep: 4 (over x).
Axes of the slice: x: 4, y: 4, z: 8, core: 2. Of those that a mesh axis runs over, the one named last changes fastest.
Arguments:
- features: bfloat16 [131072, 256], P('nodes'), may hold values from -64 to 64
- virtual_state: bfloat16 [4, 256], replicated, may hold values from -64 to 64
- w_query: bfloat16 [256, 256], P(None, 'rep'), may hold values from -0.375 to 0.375
- w_key: bfloat16 [256, 256], P(None, 'rep'), may hold values from -0.375 to 0.375
- w_value: bfloat16 [256, 256], P(None, 'rep'), may hold values from -0.375 to 0.375
- w_out: bfloat16 [256, 256], P('rep'), may hold values from -0.375 to 0.375
- tile_map: int32 [1024, 4], P('nodes'), may hold values from 0 to 1023, as said below
- local_nbr: int32 [131072, 16], P('nodes'), may hold values from 0 to 127
Outputs:
- node_out: bfloat16 [131072, 256], P('nodes', 'rep')
- virtual_out: bfloat16 [4, 256], P(None, 'rep')
The draws below stay inside these ranges and needn't reach their ends.
Inputs may be any that keep to these rules, and one draw needn't show every extreme that they name: `tile_map`: entry [c, j] is a block number. In the 16 aligned rows of one index e of nodes, the blocks numbered f * 16 to (f + 1) * 16 - 1 are named exactly 16 * 4 / 64 times, for every f.
All inputs are finite; a program needn't handle non-finite values.
Results may differ from the reference program's by a relative error of at most 0.0029.
The reference program's roundings to bfloat16 on the way (of `head_rows` and `virtual_heads`) count: a program that leaves them out, or rounds other values in their place, can miss the bound.
Values may be sent and summed in bfloat16 or wider, within the bound.
No kernel may reach another device: no remote copies, remote signals or barrier semaphores. Data moves between devices by JAX's collectives and lax.ppermute only.
A program may use at most 64 MiB of HBM per device.

```python
import math
import jax
import jax.numpy as jnp
from jax import lax

D = 256
H = 8
TILE = 128
DEG = 4
LDEG = 16
G = 4
NB_DEV = 16
NODES = 131072
N_NODES = 64


def draw_features(key, part):
    total_rows = NB_DEV * TILE * N_NODES
    key_one = jax.random.fold_in(key, 0)
    values = jnp.clip(jax.random.normal(key_one, (total_rows, D), jnp.float32), -4.0, 4.0)
    return values.astype(jnp.bfloat16)


def draw_virtual_state(key, part):
    key_one = jax.random.fold_in(key, 0)
    values = jnp.clip(jax.random.normal(key_one, (G, D), jnp.float32), -4.0, 4.0)
    return values.astype(jnp.bfloat16)


def draw_tile_map(key, part):
    key_one, key_two = jax.random.split(key, 2)
    per_peer = NB_DEV * DEG // N_NODES
    owners = jnp.repeat(jnp.arange(N_NODES, dtype=jnp.int32), per_peer)
    device_keys = jax.random.split(key_one, N_NODES)
    shuffled = jax.vmap(lambda single: jax.random.permutation(single, owners))(device_keys)
    within = jax.random.randint(key_two, (N_NODES, NB_DEV * DEG), 0, NB_DEV, jnp.int32)
    return (shuffled * NB_DEV + within).reshape(NB_DEV * N_NODES, DEG)


def plant(values, key, least, high):
    spot = [jax.random.randint(jax.random.fold_in(key, axis), (), 0, length) for axis, length in enumerate(values.shape)]
    main_axis = values.shape.index(max(values.shape))
    neighbour = spot[:main_axis] + [(spot[main_axis] + 1) % values.shape[main_axis]] + spot[main_axis + 1:]
    return values.at[tuple(spot)].set(least).at[tuple(neighbour)].set(high)


def shard_levels(rng, extent, pieces, low, largest):
    factor_of, own = 1.0, jax.random.fold_in(rng, 6)
    for axis_at, blocks in pieces:
        steps = jnp.exp(jax.random.uniform(jax.random.fold_in(own, axis_at), (blocks,), jnp.float32, low / len(pieces), largest / len(pieces)))
        factor_of = factor_of * jnp.repeat(steps, extent[axis_at] // blocks).reshape([-1 if axis == axis_at else 1 for axis in range(len(extent))])
    return factor_of


def centred(key, shape, width, bound, pieces=(), kind=jnp.bfloat16):
    array = width * jax.random.normal(key, shape, jnp.float32)
    if pieces:
        array = array * shard_levels(key, shape, pieces, -0.22, 0.18)
    return jnp.clip(array, -bound, bound).astype(kind)


def setup_inputs(seed: int = 0) -> dict:
    key_of = jax.random.split(jax.random.key(seed), 9)
    features = draw_features(jax.random.fold_in(key_of[8], 71), 0)
    virtual_state = draw_virtual_state(jax.random.fold_in(key_of[8], 71), 0)
    w_query = centred(key_of[2], (D, D), D ** -0.5, 0.375, ((1, 4),))
    w_key = centred(key_of[3], (D, D), D ** -0.5, 0.375, ((1, 4),))
    w_value = centred(key_of[4], (D, D), D ** -0.5, 0.375, ((1, 4),))
    w_out = centred(key_of[5], (D, D), D ** -0.5, 0.375, ((0, 4),))
    tile_map = draw_tile_map(jax.random.fold_in(key_of[8], 71), 0)
    local_nbr = plant(jax.random.randint(key_of[7], (NODES, LDEG), 0, TILE), jax.random.fold_in(key_of[7], 1), 0, TILE - 1).astype(jnp.int32)
    return dict(features=features, virtual_state=virtual_state, w_query=w_query, w_key=w_key, w_value=w_value, w_out=w_out, tile_map=tile_map, local_nbr=local_nbr)


def project(source, weight):
    return jnp.dot(source, weight, preferred_element_type=jnp.float32).astype(jnp.bfloat16)

def reference(features, virtual_state, w_query, w_key, w_value, w_out, tile_map, local_nbr):
    head_size = D // H
    score_scale = 1.0 / math.sqrt(head_size)
    node_count = features.shape[0]
    block_count = node_count // TILE
    queries = project(features, w_query).reshape(block_count, TILE, H, head_size)
    keys_all = project(features, w_key).reshape(block_count, TILE, H, head_size)
    values_all = project(features, w_value).reshape(block_count, TILE, H, head_size)
    virtual_queries = project(virtual_state, w_query).reshape(G, H, head_size)
    virtual_keys = project(virtual_state, w_key).reshape(G, H, head_size)
    virtual_values = project(virtual_state, w_value).reshape(G, H, head_size)
    links = local_nbr.reshape(block_count, TILE, LDEG)
    columns = jnp.arange(TILE, dtype=jnp.int32)

    def attend(block):
        neighbours = tile_map[block]
        key_rows = jnp.concatenate([keys_all[block], keys_all[neighbours].reshape(DEG * TILE, H, head_size), virtual_keys], axis=0)
        value_rows = jnp.concatenate([values_all[block], values_all[neighbours].reshape(DEG * TILE, H, head_size), virtual_values], axis=0)
        scores = jnp.einsum('qhd,khd->hqk', queries[block].astype(jnp.float32), key_rows.astype(jnp.float32), precision=lax.Precision.HIGHEST) * score_scale
        linked = jnp.any(links[block][:, :, None] == columns[None, None, :], axis=1)
        allowed = jnp.concatenate([linked, jnp.ones((TILE, DEG * TILE + G), jnp.bool_)], axis=1)
        scores = jnp.where(allowed[None], scores, -1e+30)
        highest = lax.optimization_barrier(jnp.max(scores, axis=2, keepdims=True))
        weights = jnp.exp(scores - highest)
        total_sum = lax.optimization_barrier(jnp.sum(weights, axis=2))
        rounded = lax.optimization_barrier(weights.astype(jnp.bfloat16)).astype(jnp.float32)
        blended = jnp.einsum('hqk,khd->qhd', rounded, value_rows.astype(jnp.float32), precision=lax.Precision.HIGHEST)
        blended = blended / jnp.transpose(total_sum)[..., None]
        return blended.astype(jnp.bfloat16).reshape(TILE, D)
    head_rows = lax.map(attend, jnp.arange(block_count, dtype=jnp.int32)).reshape(node_count, D)
    node_out = jnp.dot(head_rows, w_out, preferred_element_type=jnp.float32).astype(jnp.bfloat16)
    virtual_scores = jnp.einsum('ghd,nhd->hgn', virtual_queries.astype(jnp.float32), keys_all.reshape(node_count, H, head_size).astype(jnp.float32), precision=lax.Precision.HIGHEST) * score_scale
    highest = lax.optimization_barrier(jnp.max(virtual_scores, axis=2, keepdims=True))
    weights = jnp.exp(virtual_scores - highest)
    total_sum = lax.optimization_barrier(jnp.sum(weights, axis=2))
    weighted = jnp.einsum('hgn,nhd->hgd', weights, values_all.reshape(node_count, H, head_size).astype(jnp.float32), precision=lax.Precision.HIGHEST)
    virtual_heads = jnp.transpose(weighted / total_sum[..., None], (1, 0, 2)).reshape(G, D).astype(jnp.bfloat16)
    virtual_out = jnp.dot(virtual_heads, w_out, preferred_element_type=jnp.float32).astype(jnp.bfloat16)
    return (node_out, virtual_out)
```

```python
import math

import jax
import jax.numpy as jnp
from jax import lax
from jax.experimental import pallas as pl
from jax.experimental.pallas import tpu as pltpu
from jax.sharding import PartitionSpec as P

D = 256
H = 8
TILE = 128
G = 4
HEAD = D // H
REP = 4
PEERS = 64
WIDTH = D // REP
QUARTER = TILE // REP
SCORE_SCALE = 1.0 / math.sqrt(HEAD)
EXP2_SCALE = SCORE_SCALE * math.log2(math.e)
NEG = -1e30
NT = (((1,), (1,)), ((), ()))
NN = (((1,), (0,)), ((), ()))

ANY = pl.BlockSpec(memory_space=pl.ANY)
SMEM = pl.BlockSpec(memory_space=pltpu.SMEM)
VMEM = pl.BlockSpec(memory_space=pltpu.VMEM)


def dot(a, b, dims=NN, precision=None):
    return lax.dot_general(a, b, dims, precision=precision, preferred_element_type=jnp.float32)


def wanted_rows_kernel(map_ref, out_ref):
    def put(s, carry):
        block = map_ref[s // 4, s % 4]
        out_ref[block // 16] = jnp.full((1, TILE), block % 16, jnp.int32)
        return carry

    lax.fori_loop(0, PEERS, put, 0, unroll=8)


def gather_send_kernel(x_ref, want_ref, feat_ref, out_ref, sem):
    def issue(e, carry):
        pltpu.make_async_copy(feat_ref.at[want_ref[e, 0, 0] * REP + x_ref[0]], out_ref.at[e], sem).start()
        return carry

    lax.fori_loop(0, PEERS, issue, 0, unroll=8)
    pltpu.make_async_copy(out_ref, out_ref, sem).wait()


def gather_rep_kernel(x_ref, map_ref, arrived_ref, *outs_sem):
    outs, sem = outs_sem[:REP], outs_sem[REP]
    for d in range(REP):
        row = ((x_ref[0] + d) % REP) * 4

        def issue(j, carry):
            owner = map_ref[row + j // 4, j % 4] // 16
            pltpu.make_async_copy(arrived_ref.at[owner], outs[d].at[j], sem.at[d]).start()
            return carry

        lax.fori_loop(0, 16, issue, 0, unroll=8)
    for d in range(REP):
        pltpu.make_async_copy(outs[d], outs[d], sem.at[d]).wait()


def virtual_kernel(feat_ref, pack_ref, vs_ref, out_ref):
    kv = dot(feat_ref[...], pack_ref[:, :TILE]).astype(jnp.bfloat16)
    q = dot(vs_ref[...], pack_ref[:, TILE:]).astype(jnp.bfloat16)
    lane = lax.broadcasted_iota(jnp.int32, (2 * G, TILE), 1)
    row = lax.broadcasted_iota(jnp.int32, (2 * G, TILE), 0)
    first = WIDTH + HEAD * (row // G)
    q = jnp.where((lane >= first) & (lane < first + HEAD), q.astype(jnp.float32), 0.0).astype(jnp.bfloat16)
    s = dot(q, kv, NT)
    top = jnp.max(s, axis=1, keepdims=True)
    p = jnp.exp2((s - top) * EXP2_SCALE)
    total = jnp.sum(p, axis=1, keepdims=True)
    w = dot(p, kv.astype(jnp.float32), NN, lax.Precision.HIGHEST)
    out_ref[...] = jnp.where(lane < 64, w, jnp.where(lane < 96, total, top))


def attention_kernel(x_ref, *refs):
    xs, refs = refs[:2], refs[2:]
    ns, refs = (refs[:4], refs[4:8]), refs[8:]
    bias, refs = refs[:2], refs[2:]
    packs, refs = refs[:4], refs[4:]
    vs_ref, outs = refs[0], refs[1:]
    lane = lax.broadcasted_iota(jnp.int32, (TILE, TILE), 1)
    virtual_bias = jnp.where(lax.broadcasted_iota(jnp.int32, (1, TILE), 1) < G, 0.0, NEG)
    halves = []
    for half in range(2):
        own = xs[half][...]
        rows = [own] + [ns[half][d][...] for d in range(REP)] + [vs_ref[...]]
        source = jnp.concatenate(rows, axis=0)
        groups = []
        for g in range(REP):
            kv = dot(source, packs[g][:, :TILE]).astype(jnp.bfloat16)
            q = dot(own, packs[g][:, TILE:])
            q0 = jnp.where((lane >= WIDTH) & (lane < WIDTH + HEAD), q, 0.0)
            q1 = jnp.where(lane >= WIDTH + HEAD, q, 0.0)
            picked = []
            for qh in (q0, q1):
                s = dot(qh.astype(jnp.bfloat16), kv, NT)
                s = jnp.concatenate(
                    [s[:, :TILE] + bias[half][...], s[:, TILE : 5 * TILE], s[:, 5 * TILE :] + virtual_bias], axis=1
                )
                top = jnp.max(s, axis=1, keepdims=True)
                p = jnp.exp2((s - top) * EXP2_SCALE)
                total = jnp.sum(p, axis=1, keepdims=True)
                o = dot(p.astype(jnp.bfloat16), kv)
                picked.append(o * (1.0 / total))
            o = jnp.where(lane < HEAD, picked[0], jnp.where(lane < WIDTH, picked[1], 0.0))
            groups.append(o.astype(jnp.bfloat16))
        halves.append(jnp.concatenate(groups, axis=1))
    rows = jnp.concatenate(halves, axis=0)
    for d in range(REP):
        first = pl.multiple_of(((x_ref[0] + d) % REP) * WIDTH, WIDTH)
        w = jnp.concatenate([packs[g][pl.ds(first, WIDTH), TILE:] for g in range(REP)], axis=1)
        t = dot(rows, jnp.concatenate([w, w], axis=0), NT)
        outs[d][...] = jnp.where(lane < WIDTH, t[:TILE], t[TILE:]).astype(jnp.bfloat16)


def assemble_kernel(x_ref, *refs):
    out_ref = refs[REP]
    for d in range(REP):
        first = pl.multiple_of(((x_ref[0] + REP - d) % REP) * 512, 512)
        out_ref[pl.ds(first, 256), :] = refs[d][:, :WIDTH]
        out_ref[pl.ds(first + 256, 256), :] = refs[d][:, WIDTH:]


def over_rep(value):
    return [value] + [
        lax.ppermute(value, "rep", [(i, (i + d) % REP) for i in range(REP)]) for d in range(1, REP)
    ]


def send_rep(values):
    return [values[0]] + [
        lax.ppermute(values[d], "rep", [(i, (i + d) % REP) for i in range(REP)]) for d in range(1, REP)
    ]


def merged_virtual(state):
    index = lax.axis_index("nodes")
    lane = lax.broadcasted_iota(jnp.int32, state.shape, 1)
    for bit in (1, 2, 4, 8, 16, 32):
        other = lax.ppermute(state, "nodes", [(i, i ^ bit) for i in range(PEERS)])
        upper = (index & bit) != 0
        a = jnp.where(upper, other, state)
        b = jnp.where(upper, state, other)
        top_a, top_b = a[:, 96:97], b[:, 96:97]
        top = jnp.maximum(top_a, top_b)
        joined = a * jnp.exp((top_a - top) * SCORE_SCALE) + b * jnp.exp((top_b - top) * SCORE_SCALE)
        state = jnp.where(lane < 96, joined, top)
    return state


def shards(features, virtual_state, w_query, w_key, w_value, w_out, tile_map, local_nbr):
    bf16 = jnp.bfloat16
    x = lax.axis_index("rep")
    x_one = x.astype(jnp.int32).reshape(1)

    wanted_from = pl.pallas_call(
        wanted_rows_kernel,
        out_shape=jax.ShapeDtypeStruct((PEERS, 1, TILE), jnp.int32),
        in_specs=[SMEM],
        out_specs=VMEM,
        name="wanted_rows",
    )(tile_map)
    wanted = lax.all_to_all(wanted_from, "nodes", 0, 0, tiled=True)

    pack = jnp.concatenate([w_value, w_key, w_out.T, w_query], axis=1)
    packs = over_rep(pack)

    state = pl.pallas_call(
        virtual_kernel,
        out_shape=jax.ShapeDtypeStruct((2 * G, TILE), jnp.float32),
        name="virtual_part",
    )(features, pack, jnp.concatenate([virtual_state, virtual_state], axis=0))
    state = merged_virtual(state)

    outgoing = pl.pallas_call(
        gather_send_kernel,
        out_shape=jax.ShapeDtypeStruct((PEERS, QUARTER, D), bf16),
        in_specs=[SMEM, SMEM, ANY],
        out_specs=ANY,
        scratch_shapes=[pltpu.SemaphoreType.DMA],
        name="gather_send",
    )(x_one, wanted, features.reshape(PEERS, QUARTER, D))
    arrived = lax.all_to_all(outgoing, "nodes", 0, 0, tiled=True)

    sends = pl.pallas_call(
        gather_rep_kernel,
        out_shape=[jax.ShapeDtypeStruct((16, QUARTER, D), bf16)] * REP,
        in_specs=[SMEM, SMEM, ANY],
        out_specs=[ANY] * REP,
        scratch_shapes=[pltpu.SemaphoreType.DMA((REP,))],
        name="gather_rep",
    )(x_one, tile_map, arrived)
    pieces = [piece.reshape(16 * QUARTER, D) for piece in send_rep(sends)]

    own_links = lax.dynamic_slice_in_dim(local_nbr, x * 512, 512, 0)
    linked = jnp.any(own_links[:, :, None] == jnp.arange(TILE, dtype=jnp.int32), axis=1)
    bias = jnp.where(linked, 0.0, NEG).astype(jnp.float32)
    virtual_rows = jnp.pad(virtual_state, ((0, TILE - G), (0, 0)))

    tile = (TILE, D)
    low = lambda j, x: (j, 0)
    high = lambda j, x: (j + 2, 0)
    whole = lambda j, x: (0, 0)
    outs = pl.pallas_call(
        attention_kernel,
        grid_spec=pltpu.PrefetchScalarGridSpec(
            num_scalar_prefetch=1,
            grid=(2,),
            in_specs=[
                pl.BlockSpec(tile, lambda j, x: (x[0] * 4 + j, 0)),
                pl.BlockSpec(tile, lambda j, x: (x[0] * 4 + j + 2, 0)),
                *[pl.BlockSpec(tile, low)] * 4,
                *[pl.BlockSpec(tile, high)] * 4,
                pl.BlockSpec((TILE, TILE), low),
                pl.BlockSpec((TILE, TILE), high),
                *[pl.BlockSpec((D, D), whole)] * 4,
                pl.BlockSpec(tile, whole),
            ],
            out_specs=[pl.BlockSpec((TILE, TILE), low)] * 4,
        ),
        out_shape=[jax.ShapeDtypeStruct((2 * TILE, TILE), bf16)] * 4,
        name="attention",
    )(x_one, features, features, *pieces, *pieces, bias, bias, *packs, virtual_rows)
    received = send_rep(outs)
    node_out = pl.pallas_call(
        assemble_kernel,
        out_shape=jax.ShapeDtypeStruct((2048, WIDTH), bf16),
        in_specs=[SMEM] + [VMEM] * 4,
        out_specs=VMEM,
        name="assemble",
    )(x_one, *received)

    lane = lax.broadcasted_iota(jnp.int32, (G, TILE), 1)
    heads = state / state[:, 64:65]
    heads = jnp.where(lane < HEAD, heads[:G], jnp.where(lane < WIDTH, heads[G:], 0.0)).astype(bf16)
    heads_all = jnp.concatenate(over_rep(heads), axis=1)
    columns = jnp.concatenate(
        [lax.dynamic_slice(p, (x * WIDTH, TILE), (WIDTH, TILE)) for p in packs], axis=1
    )
    virtual_out = dot(heads_all, columns, NT).astype(bf16)
    return node_out, virtual_out


def solution(mesh):
    in_specs = (
        P("nodes", None),
        P(),
        P(None, "rep"),
        P(None, "rep"),
        P(None, "rep"),
        P("rep", None),
        P("nodes", None),
        P("nodes", None),
    )
    out_specs = (P("nodes", "rep"), P(None, "rep"))
    return jax.shard_map(shards, mesh=mesh, in_specs=in_specs, out_specs=out_specs, check_vma=False)
```

```python
import math

import jax
import jax.numpy as jnp
from jax import lax
from jax.experimental import pallas as pl
from jax.experimental.pallas import tpu as pltpu
from jax.sharding import PartitionSpec as P

D = 256
H = 8
TILE = 128
G = 4
HEAD = D // H
REP = 4
PEERS = 64
WIDTH = D // REP
QUARTER = TILE // REP
SCORE_SCALE = 1.0 / math.sqrt(HEAD)
EXP2_SCALE = SCORE_SCALE * math.log2(math.e)
NEG = -1e30
NT = (((1,), (1,)), ((), ()))
NN = (((1,), (0,)), ((), ()))

SMEM = pl.BlockSpec(memory_space=pltpu.SMEM)
VMEM = pl.BlockSpec(memory_space=pltpu.VMEM)
CHUNKS = 2
PER_CHUNK = 4 // CHUNKS
SLOTS = 4 * PER_CHUNK
NODES_CHUNK = TILE * PER_CHUNK
BF16 = jnp.bfloat16


def dot(a, b, dims=NN, precision=None):
    return lax.dot_general(a, b, dims, precision=precision, preferred_element_type=jnp.float32)


def in_vmem(value):
    return pltpu.with_memory_space_constraint(value, pltpu.VMEM)


def vmem_out(shape, dtype):
    return pltpu.VMEM(shape, dtype)


def params(mib):
    return pltpu.CompilerParams(vmem_limit_bytes=mib * 1024 * 1024)


def wanted_rows_kernel(map_ref, out_ref):
    def put(s, carry):
        block = map_ref[s % 4, s // 4]
        out_ref[block // 16] = jnp.full((1, TILE), block % 16, jnp.int32)
        return carry

    lax.fori_loop(0, PEERS, put, 0, unroll=8)


def gather_send_kernel(x_ref, want_ref, feat_ref, out_ref, want_smem, sem):
    copy = pltpu.make_async_copy(want_ref, want_smem, sem)
    copy.start()
    copy.wait()

    def put(e, carry):
        out_ref[e] = feat_ref[want_smem[e, 0, 0] * REP + x_ref[0]]
        return carry

    lax.fori_loop(0, PEERS, put, 0, unroll=8)


def gather_rep_kernel(x_ref, map_ref, arrived_ref, state_ref, *outs):
    for k in range(CHUNKS):
        for d in range(REP):
            column = ((x_ref[0] + d) % REP) * 4 + k * PER_CHUNK
            for j in range(SLOTS):
                owner = map_ref[j % 4, column + j // 4] // 16
                outs[k * REP + d][j] = arrived_ref[owner]
    for e in range(PEERS):
        outs[-1][e] = state_ref[...]


def prepare_kernel(x_ref, feat_ref, pack_ref, vs_ref, links_ref, state_ref, bias_ref):
    kv = dot(feat_ref[...], pack_ref[:TILE, :], NT).astype(BF16)
    q = dot(vs_ref[...], pack_ref[TILE:, :], NT).astype(BF16)
    lane = lax.broadcasted_iota(jnp.int32, (2 * G, TILE), 1)
    row = lax.broadcasted_iota(jnp.int32, (2 * G, TILE), 0)
    first = WIDTH + HEAD * (row // G)
    q = jnp.where((lane >= first) & (lane < first + HEAD), q.astype(jnp.float32), 0.0).astype(BF16)
    s = dot(q, kv, NT)
    top = jnp.max(s, axis=1, keepdims=True)
    p = jnp.exp2((s - top) * EXP2_SCALE)
    total = jnp.sum(p, axis=1, keepdims=True)
    w = dot(p, kv.astype(jnp.float32), NN, lax.Precision.HIGHEST)
    state_ref[...] = jnp.where(lane < 64, w, jnp.where(lane < 96, total, top))
    column = lax.broadcasted_iota(jnp.int32, (TILE, TILE), 0)
    for c in range(4):
        first = pl.multiple_of(x_ref[0] * 512 + c * TILE, TILE)
        links = links_ref[:, pl.ds(first, TILE)]
        linked = column == links[0:1, :]
        for n in range(1, 16):
            linked = linked | (column == links[n : n + 1, :])
        bias_ref[c * TILE : (c + 1) * TILE, :] = jnp.where(linked, 0.0, NEG).T


def attention_rows(own, source, bias, packs):
    lane = lax.broadcasted_iota(jnp.int32, (TILE, TILE), 1)
    virtual_bias = jnp.where(lax.broadcasted_iota(jnp.int32, (1, TILE), 1) < G, 0.0, NEG)
    groups = []
    for g in range(REP):
        kv = dot(source, packs[g][:TILE, :], NT).astype(BF16)
        q = dot(own, packs[g][TILE:, :], NT)
        q0 = jnp.where((lane >= WIDTH) & (lane < WIDTH + HEAD), q, 0.0)
        q1 = jnp.where(lane >= WIDTH + HEAD, q, 0.0)
        picked = []
        for qh in (q0, q1):
            s = dot(qh.astype(BF16), kv, NT)
            s = jnp.concatenate([s[:, :TILE] + bias, s[:, TILE : 5 * TILE], s[:, 5 * TILE :] + virtual_bias], axis=1)
            top = jnp.max(s, axis=1, keepdims=True)
            p = jnp.exp2((s - top) * EXP2_SCALE)
            total = jnp.sum(p, axis=1, keepdims=True)
            o = dot(p.astype(BF16), kv)
            picked.append(o * (1.0 / total))
        o = jnp.where(lane < HEAD, picked[0], jnp.where(lane < WIDTH, picked[1], 0.0))
        groups.append(o.astype(BF16))
    return jnp.concatenate(groups, axis=1)


def attention_kernel(chunk, x_ref, feat_ref, *refs):
    ns, refs = refs[:REP], refs[REP:]
    bias_ref, refs = refs[0], refs[1:]
    packs, refs = refs[:REP], refs[REP:]
    vs_ref, refs = refs[0], refs[1:]
    if chunk == CHUNKS - 1:
        states_ref, refs = refs[0], refs[1:]
    outs, scratch = refs[:REP], refs[REP]
    rows = []
    for i in range(PER_CHUNK):
        c = chunk * PER_CHUNK + i
        own = feat_ref[pl.ds(pl.multiple_of(x_ref[0] * 512 + c * TILE, TILE), TILE), :]
        near = [n[4 * i : 4 * i + 4].reshape(TILE, D) for n in ns]
        source = jnp.concatenate([own, *near, vs_ref[...]], axis=0)
        rows.append(attention_rows(own, source, bias_ref[c * TILE : (c + 1) * TILE, :], packs))
    w = jnp.concatenate([p[TILE:, :] for p in packs], axis=0)
    scratch[...] = dot(jnp.concatenate(rows, axis=0), w).T
    for d in range(REP):
        first = pl.multiple_of(((x_ref[0] + d) % REP) * WIDTH, WIDTH)
        outs[d][:WIDTH, :] = scratch[pl.ds(first, WIDTH), :].astype(BF16)
    if chunk == CHUNKS - 1:
        states = states_ref[...]
        top = jnp.max(states[:, :, 96:97], axis=0, keepdims=True)
        joined = jnp.sum(states * jnp.exp2((states[:, :, 96:97] - top) * EXP2_SCALE), axis=0)
        heads = joined * (1.0 / joined[:, WIDTH : WIDTH + 1])
        lane = lax.broadcasted_iota(jnp.int32, (G, TILE), 1)
        heads = jnp.where(lane < HEAD, heads[:G], jnp.where(lane < WIDTH, heads[G:], 0.0))
        heads = jnp.concatenate([heads, jnp.zeros((G, TILE), jnp.float32)], axis=0)
        heads = jnp.concatenate([heads, jnp.zeros((2 * G, NODES_CHUNK - TILE), jnp.float32)], axis=1)
        for d in range(REP):
            outs[d][WIDTH:, :] = heads.astype(BF16)


def assemble_kernel(x_ref, *refs):
    pieces, refs = refs[: REP * CHUNKS], refs[REP * CHUNKS :]
    packs, (out_ref, virtual_ref, scratch) = refs[:REP], refs[REP:]
    total = jnp.zeros((2 * G, D), jnp.float32)
    for d in range(REP):
        first = pl.multiple_of(((x_ref[0] + REP - d) % REP) * 512, 512)
        for k in range(CHUNKS):
            out_ref[:, pl.ds(first + k * NODES_CHUNK, NODES_CHUNK)] = pieces[k * REP + d][:WIDTH, :]
        total = total + dot(pieces[(CHUNKS - 1) * REP + d][WIDTH:, :TILE], packs[d][TILE:, :])
    scratch[...] = total.T
    virtual_ref[...] = scratch[pl.ds(pl.multiple_of(x_ref[0] * WIDTH, WIDTH), WIDTH), :].astype(BF16)


def send_rep(values, name):
    with jax.named_scope(name):
        return [values[0]] + [
            lax.ppermute(values[d], "rep", [(i, (i + d) % REP) for i in range(REP)]) for d in range(1, REP)
        ]


def shards(features, virtual_state, w_query, w_key, w_value, w_out, tile_map, local_nbr):
    x = lax.axis_index("rep")
    x_one = x.astype(jnp.int32).reshape(1)
    map_t = tile_map.T

    wanted_from = pl.pallas_call(
        wanted_rows_kernel,
        out_shape=vmem_out((PEERS, 1, TILE), jnp.int32),
        in_specs=[SMEM],
        out_specs=VMEM,
        compiler_params=params(2),
        name="wanted_rows",
    )(map_t)
    with jax.named_scope("exchange_index"):
        wanted = lax.all_to_all(wanted_from, "nodes", 0, 0, tiled=True)

    pack = jnp.concatenate([w_value.T, w_key.T, w_out, w_query.T], axis=0)
    packs = [in_vmem(p) for p in send_rep([pack] * REP, "exchange_pack")]

    state, bias = pl.pallas_call(
        prepare_kernel,
        out_shape=[vmem_out((2 * G, TILE), jnp.float32), vmem_out((512, TILE), jnp.float32)],
        in_specs=[SMEM] + [VMEM] * 4,
        out_specs=[VMEM] * 2,
        compiler_params=params(16),
        name="prepare",
    )(x_one, in_vmem(features), in_vmem(pack), jnp.concatenate([virtual_state, virtual_state], axis=0), in_vmem(local_nbr.T))

    outgoing = pl.pallas_call(
        gather_send_kernel,
        out_shape=vmem_out((PEERS, QUARTER, D), BF16),
        in_specs=[SMEM, VMEM, VMEM],
        out_specs=VMEM,
        scratch_shapes=[pltpu.SMEM((PEERS, 1, TILE), jnp.int32), pltpu.SemaphoreType.DMA],
        compiler_params=params(2),
        name="gather_send",
    )(x_one, in_vmem(wanted), in_vmem(features.reshape(PEERS, QUARTER, D)))
    with jax.named_scope("exchange_features"):
        arrived = lax.all_to_all(outgoing, "nodes", 0, 0, tiled=True)

    sends = pl.pallas_call(
        gather_rep_kernel,
        out_shape=[vmem_out((SLOTS, QUARTER, D), BF16)] * (CHUNKS * REP) + [vmem_out((PEERS, 2 * G, TILE), jnp.float32)],
        in_specs=[SMEM, SMEM, VMEM, VMEM],
        out_specs=[VMEM] * (CHUNKS * REP + 1),
        compiler_params=params(2),
        name="gather_rep",
    )(x_one, map_t, in_vmem(arrived), in_vmem(state))
    pieces = [send_rep(sends[k * REP : k * REP + REP], f"exchange_rep{k}") for k in range(CHUNKS)]
    with jax.named_scope("exchange_virtual"):
        states = lax.all_to_all(sends[-1], "nodes", 0, 0, tiled=True)

    virtual_rows = jnp.pad(virtual_state, ((0, TILE - G), (0, 0)))
    received = []
    for k in range(CHUNKS):
        last = k == CHUNKS - 1
        height = WIDTH + (2 * G if last else 0)
        args = [x_one, in_vmem(features), *map(in_vmem, pieces[k]), bias, *packs, in_vmem(virtual_rows)]
        args += [in_vmem(states)] if last else []
        outs = pl.pallas_call(
            lambda *refs, k=k: attention_kernel(k, *refs),
            out_shape=[vmem_out((height, NODES_CHUNK), BF16)] * REP,
            in_specs=[SMEM] + [VMEM] * (len(args) - 1),
            out_specs=[VMEM] * REP,
            scratch_shapes=[pltpu.VMEM((D, NODES_CHUNK), jnp.float32)],
            compiler_params=params(24),
            name=f"attention{k}",
        )(*args)
        received += send_rep(outs, f"exchange_out{k}")
    node_out, virtual_out = pl.pallas_call(
        assemble_kernel,
        out_shape=[jax.ShapeDtypeStruct((WIDTH, 2048), BF16), jax.ShapeDtypeStruct((WIDTH, 2 * G), BF16)],
        in_specs=[SMEM] + [VMEM] * (REP * CHUNKS + REP),
        out_specs=[VMEM] * 2,
        scratch_shapes=[pltpu.VMEM((D, 2 * G), jnp.float32)],
        compiler_params=params(4),
        name="assemble",
    )(x_one, *map(in_vmem, received), *packs)
    return node_out.T, virtual_out[:, :G].T


def solution(mesh):
    in_specs = (
        P("nodes", None),
        P(),
        P(None, "rep"),
        P(None, "rep"),
        P(None, "rep"),
        P("rep", None),
        P("nodes", None),
        P("nodes", None),
    )
    out_specs = (P("nodes", "rep"), P(None, "rep"))
    return jax.shard_map(shards, mesh=mesh, in_specs=in_specs, out_specs=out_specs, check_vma=False)
```

```python
import math

import jax
import jax.numpy as jnp
from jax import lax
from jax.experimental import pallas as pl
from jax.experimental.pallas import tpu as pltpu
from jax.sharding import PartitionSpec as P


D = 256
H = 8
TILE = 128
G = 4
HEAD = D // H
REP = 4
PEERS = 64
WIDTH = D // REP
QUARTER = TILE // REP
SCORE_SCALE = 1.0 / math.sqrt(HEAD)
EXP2_SCALE = SCORE_SCALE * math.log2(math.e)
NEG = -1e30
NT = (((1,), (1,)), ((), ()))
NN = (((1,), (0,)), ((), ()))

SMEM = pl.BlockSpec(memory_space=pltpu.SMEM)
VMEM = pl.BlockSpec(memory_space=pltpu.VMEM)
CHUNKS = 2
PER_CHUNK = 4 // CHUNKS
SLOTS = 4 * PER_CHUNK
NODES_CHUNK = TILE * PER_CHUNK
BF16 = jnp.bfloat16


def dot(a, b, dims=NN, precision=None):
    return lax.dot_general(a, b, dims, precision=precision, preferred_element_type=jnp.float32)


def in_vmem(value):
    return pltpu.with_memory_space_constraint(value, pltpu.VMEM)


def vmem_out(shape, dtype):
    return pltpu.VMEM(shape, dtype)


def params(mib):
    return pltpu.CompilerParams(vmem_limit_bytes=mib * 1024 * 1024)


def wanted_rows_kernel(map_ref, out_ref):
    blocks = map_ref[...]
    peer = lax.broadcasted_iota(jnp.int32, (PEERS, 16), 0)
    found = jnp.zeros((PEERS, 16), jnp.int32)
    for j in range(4):
        row = blocks[j : j + 1, :]
        found = found + jnp.where(peer == row // 16, row % 16, 0)
    out_ref[...] = jnp.broadcast_to(jnp.sum(found, axis=1, keepdims=True), (PEERS, TILE))


def gather_send_kernel(x_ref, want_ref, feat_ref, out_ref, row_ref, want_smem, sem):
    lane = lax.broadcasted_iota(jnp.int32, (PEERS, TILE), 1)
    peer = lax.broadcasted_iota(jnp.int32, (PEERS, TILE), 0)
    row_ref[...] = jnp.sum(jnp.where(lane == peer, want_ref[...], 0), axis=0, keepdims=True)
    copy = pltpu.make_async_copy(row_ref, want_smem, sem)
    copy.start()
    copy.wait()
    for e in range(PEERS):
        out_ref[e] = feat_ref[want_smem[0, e] * REP + x_ref[0]]


def gather_rep_kernel(x_ref, map_ref, arrived_ref, state_ref, *refs):
    outs = refs[REP - 1 :]
    for k in range(CHUNKS):
        for d in range(REP):
            column = ((x_ref[0] + d) % REP) * 4 + k * PER_CHUNK
            for j in range(SLOTS):
                owner = map_ref[j % 4, column + j // 4] // 16
                outs[k * REP + d][j] = arrived_ref[owner]
    for e in range(PEERS):
        outs[-1][e] = state_ref[...]


def prepare_kernel(
    x_ref, feat_in, value_ref, key_ref, out_w_ref, query_ref, vs_ref, links_ref,
    feat_ref, pack_ref, virtual_ref, state_ref, bias_ref,
):
    feat_ref[...] = feat_in[...]
    for i, part in enumerate((value_ref, key_ref, out_w_ref, query_ref)):
        pack_ref[i * WIDTH : (i + 1) * WIDTH, :] = part[...]
    vs = vs_ref[...]
    virtual_ref[...] = jnp.concatenate([vs, jnp.zeros((TILE - G, D), BF16)], axis=0)
    kv = dot(feat_in[...], pack_ref[:TILE, :], NT).astype(BF16)
    q = dot(jnp.concatenate([vs, vs], axis=0), pack_ref[TILE:, :], NT).astype(BF16)
    lane = lax.broadcasted_iota(jnp.int32, (2 * G, TILE), 1)
    row = lax.broadcasted_iota(jnp.int32, (2 * G, TILE), 0)
    first = WIDTH + HEAD * (row // G)
    q = jnp.where((lane >= first) & (lane < first + HEAD), q.astype(jnp.float32), 0.0).astype(BF16)
    s = dot(q, kv, NT)
    top = jnp.max(s, axis=1, keepdims=True)
    p = jnp.exp2((s - top) * EXP2_SCALE)
    total = jnp.sum(p, axis=1, keepdims=True)
    w = dot(p, kv.astype(jnp.float32), NN, lax.Precision.HIGHEST)
    state_ref[...] = jnp.where(lane < 64, w, jnp.where(lane < 96, total, top))
    column = lax.broadcasted_iota(jnp.int32, (TILE, TILE), 0)
    for c in range(4):
        first = pl.multiple_of(x_ref[0] * 512 + c * TILE, TILE)
        links = links_ref[:, pl.ds(first, TILE)]
        linked = column == links[0:1, :]
        for n in range(1, 16):
            linked = linked | (column == links[n : n + 1, :])
        bias_ref[c * TILE : (c + 1) * TILE, :] = jnp.where(linked, 0.0, NEG).T


def attention_rows(own, source, bias, packs, kv_ref):
    lane = lax.broadcasted_iota(jnp.int32, (TILE, TILE), 1)
    virtual_bias = jnp.where(lax.broadcasted_iota(jnp.int32, (1, TILE), 1) < G, 0.0, NEG)
    for pair in range(2):
        w = jnp.concatenate([packs[2 * pair][:TILE, :], packs[2 * pair + 1][:TILE, :]], axis=0)
        kv_ref[:, pair * D : (pair + 1) * D] = dot(source, w, NT).astype(BF16)
    q_all = dot(own, jnp.concatenate([p[TILE:, :] for p in packs], axis=0), NT)
    bias = jnp.concatenate([bias, bias], axis=0)
    groups = []
    for g in range(REP):
        q = q_all[:, g * TILE : (g + 1) * TILE]
        first = jnp.where((lane >= WIDTH) & (lane < WIDTH + HEAD), q, 0.0)
        second = jnp.where(lane >= WIDTH + HEAD, q, 0.0)
        kv = kv_ref[:, g * TILE : (g + 1) * TILE]
        s = dot(jnp.concatenate([first, second], axis=0).astype(BF16), kv, NT)
        s = jnp.concatenate([s[:, :TILE] + bias, s[:, TILE : 5 * TILE], s[:, 5 * TILE :] + virtual_bias], axis=1)
        top = jnp.max(s, axis=1, keepdims=True)
        p = jnp.exp2((s - top) * EXP2_SCALE)
        total = jnp.sum(p, axis=1, keepdims=True)
        o = dot(p.astype(BF16), kv) * (1.0 / total)
        o = jnp.where(lane < HEAD, o[:TILE], jnp.where(lane < WIDTH, o[TILE:], 0.0))
        groups.append(o.astype(BF16))
    return jnp.concatenate(groups, axis=1)


def attention_kernel(chunk, x_ref, feat_ref, *refs):
    ns, refs = refs[:REP], refs[REP:]
    bias_ref, refs = refs[0], refs[1:]
    packs, refs = refs[:REP], refs[REP:]
    vs_ref, refs = refs[0], refs[1:]
    if chunk == CHUNKS - 1:
        states_ref, refs = refs[0], refs[1:]
    outs, scratch, kv_ref = refs[:REP], refs[REP], refs[REP + 1]
    rows = []
    for i in range(PER_CHUNK):
        c = chunk * PER_CHUNK + i
        own = feat_ref[pl.ds(pl.multiple_of(x_ref[0] * 512 + c * TILE, TILE), TILE), :]
        near = [n[4 * i : 4 * i + 4].reshape(TILE, D) for n in ns]
        source = jnp.concatenate([own, *near, vs_ref[...]], axis=0)
        rows.append(attention_rows(own, source, bias_ref[c * TILE : (c + 1) * TILE, :], packs, kv_ref))
    w = jnp.concatenate([p[TILE:, :] for p in packs], axis=0)
    scratch[...] = dot(jnp.concatenate(rows, axis=0), w).T
    for d in range(REP):
        first = pl.multiple_of(((x_ref[0] + d) % REP) * WIDTH, WIDTH)
        outs[d][:WIDTH, :] = scratch[pl.ds(first, WIDTH), :].astype(BF16)
    if chunk == CHUNKS - 1:
        states = states_ref[...]
        top = jnp.max(states[:, :, 96:97], axis=0, keepdims=True)
        joined = jnp.sum(states * jnp.exp2((states[:, :, 96:97] - top) * EXP2_SCALE), axis=0)
        heads = joined * (1.0 / joined[:, WIDTH : WIDTH + 1])
        lane = lax.broadcasted_iota(jnp.int32, (G, TILE), 1)
        heads = jnp.where(lane < HEAD, heads[:G], jnp.where(lane < WIDTH, heads[G:], 0.0))
        heads = jnp.concatenate([heads, jnp.zeros((G, TILE), jnp.float32)], axis=0)
        heads = jnp.concatenate([heads, jnp.zeros((2 * G, NODES_CHUNK - TILE), jnp.float32)], axis=1)
        for d in range(REP):
            outs[d][WIDTH:, :] = heads.astype(BF16)


def assemble_kernel(x_ref, *refs):
    pieces, refs = refs[: REP * CHUNKS], refs[REP * CHUNKS :]
    packs, (out_ref, virtual_ref, scratch) = refs[:REP], refs[REP:]
    total = jnp.zeros((2 * G, D), jnp.float32)
    for d in range(REP):
        first = pl.multiple_of(((x_ref[0] + REP - d) % REP) * 512, 512)
        for k in range(CHUNKS):
            out_ref[:, pl.ds(first + k * NODES_CHUNK, NODES_CHUNK)] = pieces[k * REP + d][:WIDTH, :]
        total = total + dot(pieces[(CHUNKS - 1) * REP + d][WIDTH:, :TILE], packs[d][TILE:, :])
    scratch[...] = total.T
    own = scratch[pl.ds(pl.multiple_of(x_ref[0] * WIDTH, WIDTH), WIDTH), :]
    virtual_ref[...] = own.T[:G, :].astype(BF16)


def send_rep(values):
    return [values[0]] + [
        lax.ppermute(values[d], "rep", [(i, (i + d) % REP) for i in range(REP)]) for d in range(1, REP)
    ]


def shards(features, virtual_state, w_query, w_key, w_value, w_out, tile_map, local_nbr):
    x = lax.axis_index("rep")
    x_one = x.astype(jnp.int32).reshape(1)
    map_t = tile_map.T

    wanted_from = pl.pallas_call(
        wanted_rows_kernel,
        out_shape=vmem_out((PEERS, TILE), jnp.int32),
        in_specs=[VMEM],
        out_specs=VMEM,
        compiler_params=params(2),
        name="wanted_rows",
    )(in_vmem(map_t))
    wanted = lax.all_to_all(wanted_from.reshape(PEERS, 1, TILE), "nodes", 0, 0, tiled=True)

    rows_in_vmem, pack, virtual_rows, state, bias = pl.pallas_call(
        prepare_kernel,
        out_shape=[
            vmem_out((2048, D), BF16),
            vmem_out((D, D), BF16),
            vmem_out((TILE, D), BF16),
            vmem_out((2 * G, TILE), jnp.float32),
            vmem_out((512, TILE), jnp.float32),
        ],
        in_specs=[SMEM] + [VMEM] * 7,
        out_specs=[VMEM] * 5,
        compiler_params=params(16),
        name="prepare",
    )(x_one, features, w_value.T, w_key.T, w_out, w_query.T, virtual_state, local_nbr.T)
    packs = [in_vmem(p) for p in send_rep([pack] * REP)]

    outgoing = pl.pallas_call(
        gather_send_kernel,
        out_shape=vmem_out((PEERS, QUARTER, D), BF16),
        in_specs=[SMEM, VMEM, VMEM],
        out_specs=VMEM,
        scratch_shapes=[
            pltpu.VMEM((1, TILE), jnp.int32),
            pltpu.SMEM((1, TILE), jnp.int32),
            pltpu.SemaphoreType.DMA,
        ],
        compiler_params=params(2),
        name="gather_send",
    )(x_one, in_vmem(wanted.reshape(PEERS, TILE)), in_vmem(rows_in_vmem.reshape(PEERS, QUARTER, D)))
    arrived = lax.all_to_all(outgoing, "nodes", 0, 0, tiled=True)

    sends = pl.pallas_call(
        gather_rep_kernel,
        out_shape=[vmem_out((SLOTS, QUARTER, D), BF16)] * (CHUNKS * REP) + [vmem_out((PEERS, 2 * G, TILE), jnp.float32)],
        in_specs=[SMEM, SMEM] + [VMEM] * (REP + 1),
        out_specs=[VMEM] * (CHUNKS * REP + 1),
        compiler_params=params(2),
        name="gather_rep",
    )(x_one, map_t, in_vmem(arrived), in_vmem(state), *packs[1:])
    pieces = [send_rep(sends[k * REP : k * REP + REP]) for k in range(CHUNKS)]
    states = lax.all_to_all(sends[-1], "nodes", 0, 0, tiled=True)

    received = []
    for k in range(CHUNKS):
        last = k == CHUNKS - 1
        height = WIDTH + (2 * G if last else 0)
        args = [x_one, in_vmem(rows_in_vmem), *map(in_vmem, pieces[k]), in_vmem(bias), *packs, in_vmem(virtual_rows)]
        args += [in_vmem(states)] if last else []
        outs = pl.pallas_call(
            lambda *refs, k=k: attention_kernel(k, *refs),
            out_shape=[vmem_out((height, NODES_CHUNK), BF16)] * REP,
            in_specs=[SMEM] + [VMEM] * (len(args) - 1),
            out_specs=[VMEM] * REP,
            scratch_shapes=[pltpu.VMEM((D, NODES_CHUNK), jnp.float32), pltpu.VMEM((6 * TILE, 2 * D), BF16)],
            compiler_params=params(24),
        )(*args)
        received += send_rep(outs)
    node_out, virtual_out = pl.pallas_call(
        assemble_kernel,
        out_shape=[jax.ShapeDtypeStruct((WIDTH, 2048), BF16), jax.ShapeDtypeStruct((G, WIDTH), BF16)],
        in_specs=[SMEM] + [VMEM] * (REP * CHUNKS + REP),
        out_specs=[VMEM] * 2,
        scratch_shapes=[pltpu.VMEM((D, 2 * G), jnp.float32)],
        compiler_params=params(4),
        name="assemble",
    )(x_one, *map(in_vmem, received), *packs)
    return node_out.T, virtual_out


def solution(mesh):
    in_specs = (
        P("nodes", None),
        P(),
        P(None, "rep"),
        P(None, "rep"),
        P(None, "rep"),
        P("rep", None),
        P("nodes", None),
        P("nodes", None),
    )
    out_specs = (P("nodes", "rep"), P(None, "rep"))
    return jax.shard_map(shards, mesh=mesh, in_specs=in_specs, out_specs=out_specs, check_vma=False)
```

```python
import math

import jax
import jax.numpy as jnp
from jax import lax
from jax.experimental import pallas as pl
from jax.experimental.pallas import tpu as pltpu
from jax.sharding import PartitionSpec as P


D = 256
H = 8
TILE = 128
G = 4
HEAD = D // H
REP = 4
PEERS = 64
WIDTH = D // REP
QUARTER = TILE // REP
SCORE_SCALE = 1.0 / math.sqrt(HEAD)
EXP2_SCALE = SCORE_SCALE * math.log2(math.e)
NEG = -1e30
NT = (((1,), (1,)), ((), ()))
NN = (((1,), (0,)), ((), ()))

SMEM = pl.BlockSpec(memory_space=pltpu.SMEM)
VMEM = pl.BlockSpec(memory_space=pltpu.VMEM)
CHUNKS = 2
PER_CHUNK = 4 // CHUNKS
SLOTS = 4 * PER_CHUNK
NODES_CHUNK = TILE * PER_CHUNK
BF16 = jnp.bfloat16


def dot(a, b, dims=NN, precision=None):
    return lax.dot_general(a, b, dims, precision=precision, preferred_element_type=jnp.float32)


def in_vmem(value):
    return pltpu.with_memory_space_constraint(value, pltpu.VMEM)


def vmem_out(shape, dtype):
    return pltpu.VMEM(shape, dtype)


def params(mib):
    return pltpu.CompilerParams(vmem_limit_bytes=mib * 1024 * 1024)


def wanted_rows_kernel(map_ref, out_ref):
    blocks = map_ref[...]
    peer = lax.broadcasted_iota(jnp.int32, (PEERS, 16), 0)
    found = jnp.zeros((PEERS, 16), jnp.int32)
    for j in range(4):
        row = blocks[j : j + 1, :]
        found = found + jnp.where(peer == row // 16, row % 16, 0)
    out_ref[...] = jnp.broadcast_to(jnp.sum(found, axis=1, keepdims=True), (PEERS, TILE))


def gather_send_kernel(x_ref, want_ref, feat_ref, state_ref, out_ref, row_ref, want_smem, sem):
    lane = lax.broadcasted_iota(jnp.int32, (PEERS, TILE), 1)
    peer = lax.broadcasted_iota(jnp.int32, (PEERS, TILE), 0)
    row_ref[...] = jnp.sum(jnp.where(lane == peer, want_ref[...], 0), axis=0, keepdims=True)
    copy = pltpu.make_async_copy(row_ref, want_smem, sem)
    copy.start()
    copy.wait()
    state = state_ref[...]
    for e in range(PEERS):
        rows = feat_ref[want_smem[0, e] * REP + x_ref[0]]
        for t in range(8):
            out_ref[e, :, t * TILE : (t + 1) * TILE] = rows[t // 2 * 8 : t // 2 * 8 + 8, t % 2 * TILE : (t % 2 + 1) * TILE]
        out_ref[e, :, 8 * TILE :] = state


def gather_rep_kernel(x_ref, map_ref, arrived_ref, *refs):
    outs = refs[REP - 1 :]
    for k in range(CHUNKS):
        for d in range(REP):
            column = ((x_ref[0] + d) % REP) * 4 + k * PER_CHUNK
            for j in range(SLOTS):
                owner = map_ref[j % 4, column + j // 4] // 16
                for t in range(8):
                    piece = arrived_ref[owner, :, t * TILE : (t + 1) * TILE]
                    outs[k * REP + d][j, t // 2 * 8 : t // 2 * 8 + 8, t % 2 * TILE : (t % 2 + 1) * TILE] = piece


def thirds(value):
    high = value.astype(BF16).astype(jnp.float32)
    middle = (value - high).astype(BF16).astype(jnp.float32)
    return high, middle, value - high - middle


def join_virtual_kernel(arrived_ref, heads_ref):
    parts = arrived_ref[:, :, 8 * TILE :].astype(jnp.float32)
    flat = parts.reshape(PEERS * 2 * G, TILE)
    weighted = (flat + pltpu.roll(flat, TILE - HEAD, 1) + pltpu.roll(flat, TILE - 2 * HEAD, 1)).reshape(parts.shape)
    total = parts[:, :, 96:97] + parts[:, :, 97:98] + parts[:, :, 98:99]
    top = parts[:, :, 99:100] + parts[:, :, 100:101] + parts[:, :, 101:102]
    scale = jnp.exp2((top - jnp.max(top, axis=0, keepdims=True)) * EXP2_SCALE)
    heads = jnp.sum(weighted * scale, axis=0) * (1.0 / jnp.sum(total * scale, axis=0))
    lane = lax.broadcasted_iota(jnp.int32, (2 * G, TILE), 1)
    heads = jnp.where(lane < HEAD, heads, 0.0)
    moved = pltpu.roll(heads, HEAD, 1)
    heads_ref[...] = jnp.concatenate([heads[:G] + moved[G:], jnp.zeros((G, TILE), jnp.float32)], axis=0).astype(BF16)


def prepare_kernel(
    x_ref, feat_in, value_ref, key_ref, out_w_ref, query_ref, vs_ref, links_ref,
    feat_ref, pack_ref, virtual_ref, state_ref, bias_ref,
):
    feat_ref[...] = feat_in[...]
    for i, part in enumerate((value_ref, key_ref, out_w_ref, query_ref)):
        pack_ref[i * WIDTH : (i + 1) * WIDTH, :] = part[...]
    vs = vs_ref[...]
    virtual_ref[...] = jnp.concatenate([vs, jnp.zeros((TILE - G, D), BF16)], axis=0)
    kv = dot(feat_in[...], pack_ref[:TILE, :], NT).astype(BF16)
    q = dot(jnp.concatenate([vs, vs], axis=0), pack_ref[TILE:, :], NT).astype(BF16)
    lane = lax.broadcasted_iota(jnp.int32, (2 * G, TILE), 1)
    row = lax.broadcasted_iota(jnp.int32, (2 * G, TILE), 0)
    first = WIDTH + HEAD * (row // G)
    q = jnp.where((lane >= first) & (lane < first + HEAD), q.astype(jnp.float32), 0.0).astype(BF16)
    s = dot(q, kv, NT)
    top = jnp.max(s, axis=1, keepdims=True)
    p = jnp.exp2((s - top) * EXP2_SCALE)
    total = jnp.sum(p, axis=1, keepdims=True)
    w = dot(p, kv.astype(jnp.float32), NN, lax.Precision.HIGHEST)
    w = jnp.where(row < G, w, pltpu.roll(w, TILE - HEAD, 1))
    parts = thirds(w)
    state = jnp.where(lane < HEAD, parts[0], 0.0)
    for i in (1, 2):
        state = jnp.where((lane >= i * HEAD) & (lane < (i + 1) * HEAD), pltpu.roll(parts[i], i * HEAD, 1), state)
    for i, column in enumerate((*thirds(total), *thirds(top))):
        state = jnp.where(lane == 96 + i, column, state)
    state_ref[...] = state.astype(BF16)
    column = lax.broadcasted_iota(jnp.int32, (TILE, TILE), 0)
    for c in range(4):
        first = pl.multiple_of(x_ref[0] * 512 + c * TILE, TILE)
        links = links_ref[:, pl.ds(first, TILE)]
        linked = column == links[0:1, :]
        for n in range(1, 16):
            linked = linked | (column == links[n : n + 1, :])
        bias_ref[c * TILE : (c + 1) * TILE, :] = jnp.where(linked, 0.0, NEG).T


def attention_rows(own, source, bias, packs, kv_ref):
    lane = lax.broadcasted_iota(jnp.int32, (TILE, TILE), 1)
    virtual_bias = jnp.where(lax.broadcasted_iota(jnp.int32, (1, TILE), 1) < G, 0.0, NEG)
    for pair in range(2):
        w = jnp.concatenate([packs[2 * pair][:TILE, :], packs[2 * pair + 1][:TILE, :]], axis=0)
        kv_ref[:, pair * D : (pair + 1) * D] = dot(source, w, NT).astype(BF16)
    q_all = dot(own, jnp.concatenate([p[TILE:, :] for p in packs], axis=0), NT)
    bias = jnp.concatenate([bias, bias], axis=0)
    groups = []
    for g in range(REP):
        q = q_all[:, g * TILE : (g + 1) * TILE]
        first = jnp.where((lane >= WIDTH) & (lane < WIDTH + HEAD), q, 0.0)
        second = jnp.where(lane >= WIDTH + HEAD, q, 0.0)
        kv = kv_ref[:, g * TILE : (g + 1) * TILE]
        s = dot(jnp.concatenate([first, second], axis=0).astype(BF16), kv, NT)
        s = jnp.concatenate([s[:, :TILE] + bias, s[:, TILE : 5 * TILE], s[:, 5 * TILE :] + virtual_bias], axis=1)
        top = jnp.max(s, axis=1, keepdims=True)
        p = jnp.exp2((s - top) * EXP2_SCALE)
        total = jnp.sum(p, axis=1, keepdims=True)
        o = dot(p.astype(BF16), kv) * (1.0 / total)
        o = jnp.where(lane < HEAD, o[:TILE], jnp.where(lane < WIDTH, o[TILE:], 0.0))
        groups.append(o.astype(BF16))
    return jnp.concatenate(groups, axis=1)


def attention_kernel(chunk, x_ref, feat_ref, *refs):
    ns, refs = refs[:REP], refs[REP:]
    bias_ref, refs = refs[0], refs[1:]
    packs, refs = refs[:REP], refs[REP:]
    vs_ref, refs = refs[0], refs[1:]
    last = chunk == CHUNKS - 1
    if last:
        heads_ref, before_ref, refs = refs[0], refs[1], refs[2:]
        outs, scratch, kv_ref = refs[:REP], refs[REP], refs[REP + 1]
    else:
        rows_ref, kv_ref = refs
    rows = []
    for i in range(PER_CHUNK):
        c = chunk * PER_CHUNK + i
        own = feat_ref[pl.ds(pl.multiple_of(x_ref[0] * 512 + c * TILE, TILE), TILE), :]
        near = [n[4 * i : 4 * i + 4].reshape(TILE, D) for n in ns]
        source = jnp.concatenate([own, *near, vs_ref[...]], axis=0)
        rows.append(attention_rows(own, source, bias_ref[c * TILE : (c + 1) * TILE, :], packs, kv_ref))
    if not last:
        rows_ref[...] = jnp.concatenate(rows, axis=0)
        return
    w = jnp.concatenate([p[TILE:, :] for p in packs], axis=0)
    scratch[...] = dot(jnp.concatenate([before_ref[...], *rows], axis=0), w).T
    for d in range(REP):
        first = pl.multiple_of(((x_ref[0] + d) % REP) * WIDTH, WIDTH)
        outs[d][:WIDTH, :] = scratch[pl.ds(first, WIDTH), :].astype(BF16)
        outs[d][WIDTH:, :TILE] = heads_ref[...]
        outs[d][WIDTH:, TILE:] = jnp.zeros((2 * G, 3 * TILE), BF16)


def assemble_kernel(x_ref, *refs):
    pieces, packs, (out_ref, virtual_ref, scratch) = refs[:REP], refs[REP : 2 * REP], refs[2 * REP :]
    total = jnp.zeros((2 * G, D), jnp.float32)
    for d in range(REP):
        first = pl.multiple_of(((x_ref[0] + REP - d) % REP) * 512, 512)
        out_ref[:, pl.ds(first, 512)] = pieces[d][:WIDTH, :]
        total = total + dot(pieces[d][WIDTH:, :TILE], packs[d][TILE:, :])
    scratch[...] = total.T
    own = scratch[pl.ds(pl.multiple_of(x_ref[0] * WIDTH, WIDTH), WIDTH), :]
    virtual_ref[...] = own.T[:G, :].astype(BF16)


def send_rep(values):
    return [values[0]] + [
        lax.ppermute(values[d], "rep", [(i, (i + d) % REP) for i in range(REP)]) for d in range(1, REP)
    ]


def shards(features, virtual_state, w_query, w_key, w_value, w_out, tile_map, local_nbr):
    x = lax.axis_index("rep")
    x_one = x.astype(jnp.int32).reshape(1)
    map_t = tile_map.T

    wanted_from = pl.pallas_call(
        wanted_rows_kernel,
        out_shape=vmem_out((PEERS, TILE), jnp.int32),
        in_specs=[VMEM],
        out_specs=VMEM,
        compiler_params=params(2),
        name="wanted_rows",
    )(in_vmem(map_t))
    wanted = lax.all_to_all(wanted_from.reshape(PEERS, 1, TILE), "nodes", 0, 0, tiled=True)

    rows_in_vmem, pack, virtual_rows, state, bias = pl.pallas_call(
        prepare_kernel,
        out_shape=[
            vmem_out((2048, D), BF16),
            vmem_out((D, D), BF16),
            vmem_out((TILE, D), BF16),
            vmem_out((2 * G, TILE), BF16),
            vmem_out((512, TILE), jnp.float32),
        ],
        in_specs=[SMEM] + [VMEM] * 7,
        out_specs=[VMEM] * 5,
        compiler_params=params(16),
        name="prepare",
    )(x_one, features, w_value.T, w_key.T, w_out, w_query.T, virtual_state, local_nbr.T)
    packs = [in_vmem(p) for p in send_rep([pack] * REP)]

    outgoing = pl.pallas_call(
        gather_send_kernel,
        out_shape=vmem_out((PEERS, 8, 9 * TILE), BF16),
        in_specs=[SMEM] + [VMEM] * 3,
        out_specs=VMEM,
        scratch_shapes=[
            pltpu.VMEM((1, TILE), jnp.int32),
            pltpu.SMEM((1, TILE), jnp.int32),
            pltpu.SemaphoreType.DMA,
        ],
        compiler_params=params(2),
        name="gather_send",
    )(x_one, in_vmem(wanted.reshape(PEERS, TILE)), in_vmem(rows_in_vmem.reshape(PEERS, QUARTER, D)), in_vmem(state))
    arrived = lax.all_to_all(outgoing, "nodes", 0, 0, tiled=True)

    sends = pl.pallas_call(
        gather_rep_kernel,
        out_shape=[vmem_out((SLOTS, QUARTER, D), BF16)] * (CHUNKS * REP),
        in_specs=[SMEM, SMEM] + [VMEM] * REP,
        out_specs=[VMEM] * (CHUNKS * REP),
        compiler_params=params(2),
        name="gather_rep",
    )(x_one, map_t, in_vmem(arrived), *packs[1:])
    pieces = [send_rep(sends[k * REP : k * REP + REP]) for k in range(CHUNKS)]
    heads = pl.pallas_call(
        join_virtual_kernel,
        out_shape=vmem_out((2 * G, TILE), BF16),
        in_specs=[VMEM],
        out_specs=VMEM,
        compiler_params=params(4),
        name="join_virtual",
    )(in_vmem(arrived))

    rows = None
    for k in range(CHUNKS):
        last = k == CHUNKS - 1
        args = [x_one, in_vmem(rows_in_vmem), *map(in_vmem, pieces[k]), in_vmem(bias), *packs, in_vmem(virtual_rows)]
        args += [in_vmem(heads), in_vmem(rows)] if last else []
        if last:
            out_shape = [vmem_out((WIDTH + 2 * G, 512), BF16)] * REP
        else:
            out_shape = vmem_out((NODES_CHUNK, 2 * D), BF16)
        rows = pl.pallas_call(
            lambda *refs, k=k: attention_kernel(k, *refs),
            out_shape=out_shape,
            in_specs=[SMEM] + [VMEM] * (len(args) - 1),
            out_specs=[VMEM] * REP if last else VMEM,
            scratch_shapes=[pltpu.VMEM((D, 512), jnp.float32)] * last + [pltpu.VMEM((6 * TILE, 2 * D), BF16)],
            compiler_params=params(24),
        )(*args)
    received = send_rep(rows)
    return_shape = [jax.ShapeDtypeStruct((WIDTH, 2048), BF16), jax.ShapeDtypeStruct((G, WIDTH), BF16)]
    node_out, virtual_out = pl.pallas_call(
        assemble_kernel,
        out_shape=return_shape,
        in_specs=[SMEM] + [VMEM] * (2 * REP),
        out_specs=[VMEM] * 2,
        scratch_shapes=[pltpu.VMEM((D, 2 * G), jnp.float32)],
        compiler_params=params(4),
        name="assemble",
    )(x_one, *map(in_vmem, received), *packs)
    return node_out.T, virtual_out


def solution(mesh):
    in_specs = (
        P("nodes", None),
        P(),
        P(None, "rep"),
        P(None, "rep"),
        P(None, "rep"),
        P("rep", None),
        P("nodes", None),
        P("nodes", None),
    )
    out_specs = (P("nodes", "rep"), P(None, "rep"))
    return jax.shard_map(shards, mesh=mesh, in_specs=in_specs, out_specs=out_specs, check_vma=False)
```

```python
import math

import jax
import jax.numpy as jnp
from jax import lax
from jax.experimental import pallas as pl
from jax.experimental.pallas import tpu as pltpu
from jax.sharding import PartitionSpec as P


D = 256
H = 8
TILE = 128
G = 4
HEAD = D // H
REP = 4
PEERS = 64
WIDTH = D // REP
QUARTER = TILE // REP
SCORE_SCALE = 1.0 / math.sqrt(HEAD)
EXP2_SCALE = SCORE_SCALE * math.log2(math.e)
NEG = -1e30
NT = (((1,), (1,)), ((), ()))
NN = (((1,), (0,)), ((), ()))

SMEM = pl.BlockSpec(memory_space=pltpu.SMEM)
VMEM = pl.BlockSpec(memory_space=pltpu.VMEM)
CHUNKS = ((0, 1, 2), (3,))
KEYS = 5 * TILE + 16
PIECES = 4
BF16 = jnp.bfloat16


def dot(a, b, dims=NN, precision=None):
    return lax.dot_general(a, b, dims, precision=precision, preferred_element_type=jnp.float32)


def in_vmem(value):
    return pltpu.with_memory_space_constraint(value, pltpu.VMEM)


def in_hbm(value):
    return pltpu.with_memory_space_constraint(value, pltpu.HBM)


def vmem_out(shape, dtype):
    return pltpu.VMEM(shape, dtype)


def params(mib):
    return pltpu.CompilerParams(vmem_limit_bytes=mib * 1024 * 1024)


def wanted_rows_kernel(map_ref, out_ref):
    blocks = map_ref[...]
    peer = lax.broadcasted_iota(jnp.int32, (PEERS, 16), 0)
    found = jnp.zeros((PEERS, 16), jnp.int32)
    for j in range(4):
        row = blocks[j : j + 1, :]
        found = found + jnp.where(peer == row // 16, row % 16, 0)
    out_ref[...] = jnp.broadcast_to(jnp.sum(found, axis=1, keepdims=True), (PEERS, TILE))


def gather_send_kernel(want_ref, feat_ref, state_ref, out_ref, row_ref, want_smem, sem):
    lane = lax.broadcasted_iota(jnp.int32, (PEERS, TILE), 1)
    peer = lax.broadcasted_iota(jnp.int32, (PEERS, TILE), 0)
    row_ref[...] = jnp.sum(jnp.where(lane == peer, want_ref[...], 0), axis=0, keepdims=True)
    copy = pltpu.make_async_copy(row_ref, want_smem, sem)
    copy.start()
    copy.wait()
    state = state_ref[...]
    for e in range(PEERS):
        rows = feat_ref[want_smem[0, e] * REP + lax.axis_index("rep")]
        for t in range(8):
            out_ref[e, :, t * TILE : (t + 1) * TILE] = rows[t // 2 * 8 : t // 2 * 8 + 8, t % 2 * TILE : (t % 2 + 1) * TILE]
        out_ref[e, :, 8 * TILE :] = state


def gather_rep_kernel(map_ref, arrived_ref, *refs):
    outs = refs[REP - 1 :]
    for k, blocks in enumerate(CHUNKS):
        for d in range(REP):
            column = ((lax.axis_index("rep") + d) % REP) * 4 + blocks[0]
            for j in range(4 * len(blocks)):
                owner = map_ref[j % 4, column + j // 4] // 16
                for t in range(8):
                    piece = arrived_ref[owner, :, t * TILE : (t + 1) * TILE]
                    outs[k * REP + d][j, t // 2 * 8 : t // 2 * 8 + 8, t % 2 * TILE : (t % 2 + 1) * TILE] = piece


def thirds(value):
    high = value.astype(BF16).astype(jnp.float32)
    middle = (value - high).astype(BF16).astype(jnp.float32)
    return high, middle, value - high - middle


def join_virtual_kernel(arrived_ref, heads_ref):
    parts = arrived_ref[:, :, 8 * TILE :].astype(jnp.float32)
    flat = parts.reshape(PEERS * 2 * G, TILE)
    weighted = (flat + pltpu.roll(flat, TILE - HEAD, 1) + pltpu.roll(flat, TILE - 2 * HEAD, 1)).reshape(parts.shape)
    total = parts[:, :, 96:97] + parts[:, :, 97:98] + parts[:, :, 98:99]
    top = parts[:, :, 99:100] + parts[:, :, 100:101] + parts[:, :, 101:102]
    scale = jnp.exp2((top - jnp.max(top, axis=0, keepdims=True)) * EXP2_SCALE)
    heads = jnp.sum(weighted * scale, axis=0) * (1.0 / jnp.sum(total * scale, axis=0))
    lane = lax.broadcasted_iota(jnp.int32, (2 * G, TILE), 1)
    heads = jnp.where(lane < HEAD, heads, 0.0)
    moved = pltpu.roll(heads, HEAD, 1)
    heads_ref[...] = jnp.concatenate([heads[:G] + moved[G:], jnp.zeros((G, TILE), jnp.float32)], axis=0).astype(BF16)


def prepare_kernel(
    feat_in, value_in, key_in, out_in, query_in, vs_ref, feat_ref, pack_ref, virtual_ref, state_ref, sems
):
    copies = [
        pltpu.make_async_copy(part, pack_ref.at[i * WIDTH : (i + 1) * WIDTH], sems.at[i])
        for i, part in enumerate((value_in, key_in, out_in, query_in))
    ]
    size = 2048 // PIECES
    for i in range(PIECES):
        rows = slice(i * size, (i + 1) * size)
        copies.append(pltpu.make_async_copy(feat_in.at[rows], feat_ref.at[rows], sems.at[4 + i]))
    for copy in copies:
        copy.start()
    vs = vs_ref[...]
    virtual_ref[...] = jnp.concatenate([vs, jnp.zeros((TILE - G, D), BF16)], axis=0)
    for copy in copies[:4]:
        copy.wait()
    q = dot(jnp.concatenate([vs, vs], axis=0), pack_ref[TILE:, :], NT)
    lane = lax.broadcasted_iota(jnp.int32, (2 * G, TILE), 1)
    row = lax.broadcasted_iota(jnp.int32, (2 * G, TILE), 0)
    first = WIDTH + HEAD * (row // G)
    q = jnp.where((lane >= first) & (lane < first + HEAD), q, 0.0).astype(BF16)
    weights = pack_ref[:TILE, :]
    kv, s = [], []
    for i in range(PIECES):
        copies[4 + i].wait()
        kv.append(dot(feat_ref[i * size : (i + 1) * size, :], weights, NT).astype(BF16))
        s.append(dot(q, kv[i], NT))
    s = jnp.concatenate(s, axis=1)
    top = jnp.max(s, axis=1, keepdims=True)
    p = jnp.exp2((s - top) * EXP2_SCALE)
    total = jnp.sum(p, axis=1, keepdims=True)
    w = dot(jnp.concatenate(thirds(p), axis=0).astype(BF16), jnp.concatenate(kv, axis=0))
    w = w[: 2 * G] + w[2 * G : 4 * G] + w[4 * G :]
    w = jnp.where(row < G, w, pltpu.roll(w, TILE - HEAD, 1))
    parts = thirds(w)
    state = jnp.where(lane < HEAD, parts[0], 0.0)
    for i in (1, 2):
        state = jnp.where((lane >= i * HEAD) & (lane < (i + 1) * HEAD), pltpu.roll(parts[i], i * HEAD, 1), state)
    for i, column in enumerate((*thirds(total), *thirds(top))):
        state = jnp.where(lane == 96 + i, column, state)
    state_ref[...] = state.astype(BF16)


def masks_kernel(links_ref, bias_ref):
    position = lax.broadcasted_iota(jnp.int32, (TILE, TILE), 0)
    for c in range(4):
        first = pl.multiple_of(lax.axis_index("rep") * 512 + c * TILE, TILE)
        links = links_ref[:, pl.ds(first, TILE)]
        linked = position == links[0:1, :]
        for n in range(1, 16):
            linked = linked | (position == links[n : n + 1, :])
        bias_ref[:, c * TILE : (c + 1) * TILE] = jnp.where(linked, 0.0, NEG)


def attention(blocks, feat_ref, ns, bias_ref, packs, vs_ref, key_ref, value_ref, score_ref, weight_ref, query_ref):
    lane = lax.broadcasted_iota(jnp.int32, (TILE, TILE), 1)
    row = lax.broadcasted_iota(jnp.int32, (16, 2 * TILE), 0)
    w_value = jnp.concatenate([p[:WIDTH, :] for p in packs], axis=0)
    w_key = jnp.concatenate([p[WIDTH : 2 * WIDTH, :] for p in packs], axis=0)
    w_query = jnp.concatenate([p[3 * WIDTH :, :] for p in packs], axis=0)
    for b in range(2):
        weight_ref[b, KEYS:, :] = jnp.zeros((6 * TILE - KEYS, 2 * TILE), BF16)

    def project(i):
        first = pl.multiple_of(lax.axis_index("rep") * 512 + blocks[i] * TILE, TILE)
        own = feat_ref[pl.ds(first, TILE), :]
        near = [n[4 * i : 4 * i + 4].reshape(TILE, D) for n in ns]
        key_ref[i] = dot(jnp.concatenate([own, *near, vs_ref[:16, :]], axis=0), w_key, NT).astype(BF16)
        value_ref[i] = dot(w_value, jnp.concatenate([own, *near, vs_ref[...]], axis=0), NT).astype(BF16)
        q = dot(own, w_query, NT)
        for pair in range(4):
            part = q[:, pair // 2 * TILE : (pair // 2 + 1) * TILE]
            for k in range(2):
                low = (2 * pair + k) % 4 * HEAD
                masked = jnp.where((lane >= low) & (lane < low + HEAD), part, 0.0).astype(BF16)
                query_ref[i, pair, k * TILE : (k + 1) * TILE, :] = masked

    def score(n):
        i, pair = divmod(n, 4)
        s = dot(key_ref[i, :, pair // 2 * TILE : (pair // 2 + 1) * TILE], query_ref[i, pair], NT)
        bias = bias_ref[:, blocks[i] * TILE : (blocks[i] + 1) * TILE]
        bias = jnp.concatenate([bias, bias], axis=1)
        near, far = s[:TILE] + bias, jnp.where(row < G, s[5 * TILE :], NEG)
        score_ref[n % 2] = jnp.concatenate([near, s[TILE : 5 * TILE], far], axis=0)

    def weigh(n):
        s = score_ref[n % 2]
        p = jnp.exp2((s - jnp.max(s, axis=0, keepdims=True)) * EXP2_SCALE)
        weight_ref[n % 2, :KEYS, :] = p.astype(BF16)
        return 1.0 / jnp.sum(p, axis=0, keepdims=True)

    def blend(n, scale):
        i, pair = divmod(n, 4)
        o = dot(value_ref[i, pair * WIDTH : (pair + 1) * WIDTH, :], weight_ref[n % 2]) * scale
        return jnp.concatenate([o[:HEAD, :TILE], o[HEAD:, TILE:]], axis=0)

    project(0)
    score(0)
    parts, scale = [], None
    for n in range(4 * len(blocks)):
        if n % 4 == 1 and n // 4 + 1 < len(blocks):
            project(n // 4 + 1)
        if n + 1 < 4 * len(blocks):
            score(n + 1)
        if n:
            parts.append(blend(n - 1, scale))
        scale = weigh(n)
    parts.append(blend(4 * len(blocks) - 1, scale))
    heads = [jnp.concatenate(parts[4 * i : 4 * i + 4], axis=0) for i in range(len(blocks))]
    w_out = jnp.concatenate([p[2 * WIDTH : 3 * WIDTH, :] for p in packs], axis=0)
    return dot(w_out, jnp.concatenate(heads, axis=1).astype(BF16), (((0,), (0,)), ((), ()))).astype(BF16)


def attention_kernel(chunk, feat_ref, *refs):
    ns, refs = refs[:REP], refs[REP:]
    bias_ref, refs = refs[0], refs[1:]
    packs, refs = refs[:REP], refs[REP:]
    vs_ref, refs = refs[0], refs[1:]
    refs, scratch = refs[:-5], refs[-5:]
    out = attention(CHUNKS[chunk], feat_ref, ns, bias_ref, packs, vs_ref, *scratch)
    if chunk == 0:
        refs[0][...] = out
        return
    heads_ref, before_ref, *outs, own_ref = refs
    own_ref[...] = out
    done = before_ref.shape[1]
    for d in range(REP):
        first = pl.multiple_of(((lax.axis_index("rep") + d) % REP) * WIDTH, WIDTH)
        outs[d][:WIDTH, :done] = before_ref[pl.ds(first, WIDTH), :]
        outs[d][:WIDTH, done:] = own_ref[pl.ds(first, WIDTH), :]
        outs[d][WIDTH:, :TILE] = heads_ref[...]
        outs[d][WIDTH:, TILE:] = jnp.zeros((2 * G, 3 * TILE), BF16)


def assemble_kernel(*refs):
    pieces, packs, (out_ref, virtual_ref, scratch) = refs[:REP], refs[REP : 2 * REP], refs[2 * REP :]
    total = jnp.zeros((2 * G, D), jnp.float32)
    for d in range(REP):
        first = pl.multiple_of(((lax.axis_index("rep") + REP - d) % REP) * 512, 512)
        out_ref[:, pl.ds(first, 512)] = pieces[d][:WIDTH, :]
        total = total + dot(pieces[d][WIDTH:, :TILE], packs[d][TILE:, :])
    scratch[...] = total.T
    own = scratch[pl.ds(pl.multiple_of(lax.axis_index("rep") * WIDTH, WIDTH), WIDTH), :]
    virtual_ref[...] = own.T[:G, :].astype(BF16)


def send_rep(values):
    return [values[0]] + [
        lax.ppermute(values[d], "rep", [(i, (i + d) % REP) for i in range(REP)]) for d in range(1, REP)
    ]


def shards(features, virtual_state, w_query, w_key, w_value, w_out, tile_map, local_nbr):
    map_t = tile_map.T

    wanted_from = pl.pallas_call(
        wanted_rows_kernel,
        out_shape=vmem_out((PEERS, TILE), jnp.int32),
        in_specs=[VMEM],
        out_specs=VMEM,
        compiler_params=params(2),
        name="wanted_rows",
    )(in_vmem(map_t))
    wanted = lax.all_to_all(wanted_from.reshape(PEERS, 1, TILE), "nodes", 0, 0, tiled=True)

    rows_in_vmem, pack, virtual_rows, state = pl.pallas_call(
        prepare_kernel,
        out_shape=[
            vmem_out((2048, D), BF16),
            vmem_out((D, D), BF16),
            vmem_out((TILE, D), BF16),
            vmem_out((2 * G, TILE), BF16),
        ],
        in_specs=[pl.BlockSpec(memory_space=pl.ANY)] * 5 + [VMEM],
        out_specs=[VMEM] * 4,
        scratch_shapes=[pltpu.SemaphoreType.DMA((4 + PIECES,))],
        compiler_params=params(16),
        name="prepare",
    )(*map(in_hbm, (features, w_value.T, w_key.T, w_out, w_query.T)), virtual_state)
    bias = pl.pallas_call(
        masks_kernel,
        out_shape=vmem_out((TILE, 512), jnp.float32),
        in_specs=[VMEM],
        out_specs=VMEM,
        compiler_params=params(2),
        name="masks",
    )(local_nbr.T)
    packs = [in_vmem(p) for p in send_rep([pack] * REP)]

    outgoing = pl.pallas_call(
        gather_send_kernel,
        out_shape=vmem_out((PEERS, 8, 9 * TILE), BF16),
        in_specs=[VMEM] * 3,
        out_specs=VMEM,
        scratch_shapes=[
            pltpu.VMEM((1, TILE), jnp.int32),
            pltpu.SMEM((1, TILE), jnp.int32),
            pltpu.SemaphoreType.DMA,
        ],
        compiler_params=params(2),
        name="gather_send",
    )(in_vmem(wanted.reshape(PEERS, TILE)), in_vmem(rows_in_vmem.reshape(PEERS, QUARTER, D)), in_vmem(state))
    arrived = lax.all_to_all(outgoing, "nodes", 0, 0, tiled=True)

    sends = pl.pallas_call(
        gather_rep_kernel,
        out_shape=[vmem_out((4 * len(blocks), QUARTER, D), BF16) for blocks in CHUNKS for _ in range(REP)],
        in_specs=[SMEM] + [VMEM] * REP,
        out_specs=[VMEM] * (len(CHUNKS) * REP),
        compiler_params=params(2),
        name="gather_rep",
    )(map_t, in_vmem(arrived), *packs[1:])
    pieces = [send_rep(sends[k * REP : k * REP + REP]) for k in range(len(CHUNKS))]
    heads = pl.pallas_call(
        join_virtual_kernel,
        out_shape=vmem_out((2 * G, TILE), BF16),
        in_specs=[VMEM],
        out_specs=VMEM,
        compiler_params=params(4),
        name="join_virtual",
    )(in_vmem(arrived))

    rows = None
    for k, blocks in enumerate(CHUNKS):
        last = k == len(CHUNKS) - 1
        args = [in_vmem(rows_in_vmem), *map(in_vmem, pieces[k]), in_vmem(bias), *packs, in_vmem(virtual_rows)]
        args += [in_vmem(heads), in_vmem(rows)] if last else []
        count = len(blocks)
        rows = pl.pallas_call(
            lambda *refs, k=k: attention_kernel(k, *refs),
            out_shape=[vmem_out((WIDTH + 2 * G, 512), BF16)] * REP if last else vmem_out((D, count * TILE), BF16),
            in_specs=[VMEM] * len(args),
            out_specs=[VMEM] * REP if last else VMEM,
            scratch_shapes=[pltpu.VMEM((D, TILE), BF16)] * last
            + [
                pltpu.VMEM((count, KEYS, D), BF16),
                pltpu.VMEM((count, D, 6 * TILE), BF16),
                pltpu.VMEM((2, KEYS, 2 * TILE), jnp.float32),
                pltpu.VMEM((2, 6 * TILE, 2 * TILE), BF16),
                pltpu.VMEM((count, 4, 2 * TILE, TILE), BF16),
            ],
            compiler_params=params(24),
        )(*args)
    received = send_rep(rows)
    return_shape = [jax.ShapeDtypeStruct((WIDTH, 2048), BF16), jax.ShapeDtypeStruct((G, WIDTH), BF16)]
    node_out, virtual_out = pl.pallas_call(
        assemble_kernel,
        out_shape=return_shape,
        in_specs=[VMEM] * (2 * REP),
        out_specs=[VMEM] * 2,
        scratch_shapes=[pltpu.VMEM((D, 2 * G), jnp.float32)],
        compiler_params=params(4),
        name="assemble",
    )(*map(in_vmem, received), *packs)
    return node_out.T, virtual_out


def solution(mesh):
    in_specs = (
        P("nodes", None),
        P(),
        P(None, "rep"),
        P(None, "rep"),
        P(None, "rep"),
        P("rep", None),
        P("nodes", None),
        P("nodes", None),
    )
    out_specs = (P("nodes", "rep"), P(None, "rep"))
    return jax.shard_map(shards, mesh=mesh, in_specs=in_specs, out_specs=out_specs, check_vma=False)
```

```python
import math

import jax
import jax.numpy as jnp
from jax import lax
from jax.experimental import pallas as pl
from jax.experimental.pallas import tpu as pltpu
from jax.sharding import PartitionSpec as P


D = 256
H = 8
TILE = 128
G = 4
HEAD = D // H
REP = 4
PEERS = 64
WIDTH = D // REP
QUARTER = TILE // REP
SCORE_SCALE = 1.0 / math.sqrt(HEAD)
EXP2_SCALE = SCORE_SCALE * math.log2(math.e)
NEG = -1e30
NT = (((1,), (1,)), ((), ()))
NN = (((1,), (0,)), ((), ()))

SMEM = pl.BlockSpec(memory_space=pltpu.SMEM)
VMEM = pl.BlockSpec(memory_space=pltpu.VMEM)
CHUNKS = ((0, 1), (2, 3))
NEAR = 4 * TILE
OWN = TILE + 16
PIECES = 4
BF16 = jnp.bfloat16


def dot(a, b, dims=NN, precision=None):
    return lax.dot_general(a, b, dims, precision=precision, preferred_element_type=jnp.float32)


def in_vmem(value):
    return pltpu.with_memory_space_constraint(value, pltpu.VMEM)


def in_hbm(value):
    return pltpu.with_memory_space_constraint(value, pltpu.HBM)


def vmem_out(shape, dtype):
    return pltpu.VMEM(shape, dtype)


def params(mib):
    return pltpu.CompilerParams(vmem_limit_bytes=mib * 1024 * 1024)


def wanted_rows_kernel(map_ref, out_ref):
    blocks = map_ref[...]
    peer = lax.broadcasted_iota(jnp.int32, (PEERS, 16), 0)
    found = jnp.zeros((PEERS, 16), jnp.int32)
    for j in range(4):
        row = blocks[j : j + 1, :]
        found = found + jnp.where(peer == row // 16, row % 16, 0)
    out_ref[...] = jnp.broadcast_to(jnp.sum(found, axis=1, keepdims=True), (PEERS, TILE))


def gather_send_kernel(want_ref, feat_ref, state_ref, out_ref):
    state = state_ref[...]
    for e in range(PEERS):
        rows = feat_ref[want_ref[e : e + 1, :][0, 0] * REP + lax.axis_index("rep")]
        for t in range(8):
            out_ref[e, :, t * TILE : (t + 1) * TILE] = rows[t // 2 * 8 : t // 2 * 8 + 8, t % 2 * TILE : (t % 2 + 1) * TILE]
        out_ref[e, :, 8 * TILE :] = state


def gather_rep_kernel(map_ref, arrived_ref, *refs):
    outs = refs[REP - 1 :]
    for k, blocks in enumerate(CHUNKS):
        for d in range(REP):
            column = ((lax.axis_index("rep") + d) % REP) * 4 + blocks[0]
            for j in range(4 * len(blocks)):
                owner = map_ref[j % 4, column + j // 4] // 16
                for t in range(8):
                    piece = arrived_ref[owner, :, t * TILE : (t + 1) * TILE]
                    outs[k * REP + d][j, t // 2 * 8 : t // 2 * 8 + 8, t % 2 * TILE : (t % 2 + 1) * TILE] = piece


def thirds(value):
    high = value.astype(BF16).astype(jnp.float32)
    middle = (value - high).astype(BF16).astype(jnp.float32)
    return high, middle, value - high - middle


def join_virtual_kernel(arrived_ref, heads_ref):
    parts = arrived_ref[:, :, 8 * TILE :].astype(jnp.float32)
    flat = parts.reshape(PEERS * 2 * G, TILE)
    weighted = (flat + pltpu.roll(flat, TILE - HEAD, 1) + pltpu.roll(flat, TILE - 2 * HEAD, 1)).reshape(parts.shape)
    total = parts[:, :, 96:97] + parts[:, :, 97:98] + parts[:, :, 98:99]
    top = parts[:, :, 99:100] + parts[:, :, 100:101] + parts[:, :, 101:102]
    scale = jnp.exp2((top - jnp.max(top, axis=0, keepdims=True)) * EXP2_SCALE)
    heads = jnp.sum(weighted * scale, axis=0) * (1.0 / jnp.sum(total * scale, axis=0))
    lane = lax.broadcasted_iota(jnp.int32, (2 * G, TILE), 1)
    heads = jnp.where(lane < HEAD, heads, 0.0)
    moved = pltpu.roll(heads, HEAD, 1)
    heads_ref[...] = jnp.concatenate([heads[:G] + moved[G:], jnp.zeros((G, TILE), jnp.float32)], axis=0).astype(BF16)


def prepare_kernel(
    feat_in, value_in, key_in, out_in, query_in, vs_ref, feat_ref, pack_ref, virtual_ref, state_ref, sems
):
    copies = [
        pltpu.make_async_copy(part, pack_ref.at[i * WIDTH : (i + 1) * WIDTH], sems.at[i])
        for i, part in enumerate((value_in, key_in, out_in, query_in))
    ]
    size = 2048 // PIECES
    for i in range(PIECES):
        rows = slice(i * size, (i + 1) * size)
        copies.append(pltpu.make_async_copy(feat_in.at[rows], feat_ref.at[rows], sems.at[4 + i]))
    for copy in copies:
        copy.start()
    vs = vs_ref[...]
    virtual_ref[...] = jnp.concatenate([vs, jnp.zeros((TILE - G, D), BF16)], axis=0)
    for copy in copies[:4]:
        copy.wait()
    q = dot(jnp.concatenate([vs, vs], axis=0), pack_ref[TILE:, :], NT)
    lane = lax.broadcasted_iota(jnp.int32, (2 * G, TILE), 1)
    row = lax.broadcasted_iota(jnp.int32, (2 * G, TILE), 0)
    first = WIDTH + HEAD * (row // G)
    q = jnp.where((lane >= first) & (lane < first + HEAD), q, 0.0).astype(BF16)
    weights = pack_ref[:TILE, :]
    kv, s = [], []
    for i in range(PIECES):
        copies[4 + i].wait()
        kv.append(dot(feat_ref[i * size : (i + 1) * size, :], weights, NT).astype(BF16))
        s.append(dot(q, kv[i], NT))
    s = jnp.concatenate(s, axis=1)
    top = jnp.max(s, axis=1, keepdims=True)
    p = jnp.exp2((s - top) * EXP2_SCALE)
    total = jnp.sum(p, axis=1, keepdims=True)
    w = dot(jnp.concatenate(thirds(p), axis=0).astype(BF16), jnp.concatenate(kv, axis=0))
    w = w[: 2 * G] + w[2 * G : 4 * G] + w[4 * G :]
    w = jnp.where(row < G, w, pltpu.roll(w, TILE - HEAD, 1))
    parts = thirds(w)
    state = jnp.where(lane < HEAD, parts[0], 0.0)
    for i in (1, 2):
        state = jnp.where((lane >= i * HEAD) & (lane < (i + 1) * HEAD), pltpu.roll(parts[i], i * HEAD, 1), state)
    for i, column in enumerate((*thirds(total), *thirds(top))):
        state = jnp.where(lane == 96 + i, column, state)
    state_ref[...] = state.astype(BF16)


def own_part_kernel(feat_ref, links_ref, vs_ref, *refs):
    packs, (query_ref, score_ref, value_ref, w_out_ref) = refs[:REP], refs[REP:]
    lane = lax.broadcasted_iota(jnp.int32, (TILE, TILE), 1)
    row = lax.broadcasted_iota(jnp.int32, (16, 2 * TILE), 0)
    position = lax.broadcasted_iota(jnp.int32, (TILE, TILE), 0)
    w_value = jnp.concatenate([p[:WIDTH, :] for p in packs], axis=0)
    w_key = jnp.concatenate([p[WIDTH : 2 * WIDTH, :] for p in packs], axis=0)
    w_query = jnp.concatenate([p[3 * WIDTH :, :] for p in packs], axis=0)
    w_out = jnp.concatenate([p[2 * WIDTH : 3 * WIDTH, :] for p in packs], axis=0)
    w_out_ref[...] = w_out.astype(jnp.float32).T.astype(BF16)
    for c in range(4):
        first = pl.multiple_of(lax.axis_index("rep") * 512 + c * TILE, TILE)
        links = links_ref[:, pl.ds(first, TILE)]
        linked = position == links[0:1, :]
        for n in range(1, 16):
            linked = linked | (position == links[n : n + 1, :])
        bias = jnp.where(linked, 0.0, NEG)
        bias = jnp.concatenate([bias, bias], axis=1)
        own = feat_ref[pl.ds(first, TILE), :]
        keys = dot(jnp.concatenate([own, vs_ref[:16, :]], axis=0), w_key, NT).astype(BF16)
        value_ref[c] = dot(w_value, jnp.concatenate([own, vs_ref[...]], axis=0), NT).astype(BF16)
        q = dot(own, w_query, NT)
        for pair in range(4):
            part = slice(pair // 2 * TILE, (pair // 2 + 1) * TILE)
            for k in range(2):
                low = (2 * pair + k) % 4 * HEAD
                masked = jnp.where((lane >= low) & (lane < low + HEAD), q[:, part], 0.0).astype(BF16)
                query_ref[c, pair, k * TILE : (k + 1) * TILE, :] = masked
            s = dot(keys[:, part], query_ref[c, pair], NT)
            score_ref[c, pair] = jnp.concatenate([s[:TILE] + bias, jnp.where(row < G, s[TILE:], NEG)], axis=0)


def attention(blocks, ns, own, packs, key_ref, value_ref, score_ref, weight_ref):
    query_ref, own_score_ref, own_value_ref, w_out_ref = own
    w_value = jnp.concatenate([p[:WIDTH, :] for p in packs], axis=0)
    w_key = jnp.concatenate([p[WIDTH : 2 * WIDTH, :] for p in packs], axis=0)
    for b in range(2):
        weight_ref[b, OWN : 2 * TILE, :] = jnp.zeros((2 * TILE - OWN, 2 * TILE), BF16)

    def project(i):
        near = jnp.concatenate([n[4 * i : 4 * i + 4].reshape(TILE, D) for n in ns], axis=0)
        key_ref[i] = dot(near, w_key, NT).astype(BF16)
        value_ref[i] = dot(w_value, near, NT).astype(BF16)

    def score(n):
        i, pair = divmod(n, 4)
        keys = key_ref[i, :, pair // 2 * TILE : (pair // 2 + 1) * TILE]
        score_ref[n % 2] = dot(keys, query_ref[blocks[i], pair], NT)

    def weigh(n):
        i, pair = divmod(n, 4)
        s, own_s = score_ref[n % 2], own_score_ref[blocks[i], pair]
        top = jnp.maximum(jnp.max(s, axis=0, keepdims=True), jnp.max(own_s, axis=0, keepdims=True))
        p = jnp.exp2((s - top) * EXP2_SCALE)
        own_p = jnp.exp2((own_s - top) * EXP2_SCALE)
        weight_ref[n % 2, :OWN, :] = own_p.astype(BF16)
        weight_ref[n % 2, 2 * TILE :, :] = p.astype(BF16)
        return 1.0 / (jnp.sum(p, axis=0, keepdims=True) + jnp.sum(own_p, axis=0, keepdims=True))

    def blend(n, scale):
        i, pair = divmod(n, 4)
        rows = slice(pair * WIDTH, (pair + 1) * WIDTH)
        values = jnp.concatenate([own_value_ref[blocks[i], rows, :], value_ref[i, rows, :]], axis=1)
        o = dot(values, weight_ref[n % 2]) * scale
        return jnp.concatenate([o[:HEAD, :TILE], o[HEAD:, TILE:]], axis=0)

    project(0)
    score(0)
    parts, scale = [], None
    for n in range(4 * len(blocks)):
        if n % 4 == 1 and n // 4 + 1 < len(blocks):
            project(n // 4 + 1)
        if n + 1 < 4 * len(blocks):
            score(n + 1)
        if n:
            parts.append(blend(n - 1, scale))
        scale = weigh(n)
    parts.append(blend(4 * len(blocks) - 1, scale))
    heads = [jnp.concatenate(parts[4 * i : 4 * i + 4], axis=0) for i in range(len(blocks))]
    return dot(w_out_ref[...], jnp.concatenate(heads, axis=1).astype(BF16)).astype(BF16)


def attention_kernel(chunk, *refs):
    ns, own, packs, refs = refs[:REP], refs[REP : 2 * REP], refs[2 * REP : 3 * REP], refs[3 * REP :]
    refs, scratch = refs[:-4], refs[-4:]
    out = attention(CHUNKS[chunk], ns, own, packs, *scratch)
    if chunk == 0:
        refs[0][...] = out
        return
    heads_ref, before_ref, *outs, own_ref = refs
    own_ref[...] = out
    done = before_ref.shape[1]
    for d in range(REP):
        first = pl.multiple_of(((lax.axis_index("rep") + d) % REP) * WIDTH, WIDTH)
        outs[d][:WIDTH, :done] = before_ref[pl.ds(first, WIDTH), :]
        outs[d][:WIDTH, done:] = own_ref[pl.ds(first, WIDTH), :]
        outs[d][WIDTH:, :TILE] = heads_ref[...]
        outs[d][WIDTH:, TILE:] = jnp.zeros((2 * G, 3 * TILE), BF16)


def assemble_kernel(*refs):
    pieces, packs, (out_ref, virtual_ref, scratch) = refs[:REP], refs[REP : 2 * REP], refs[2 * REP :]
    total = jnp.zeros((2 * G, D), jnp.float32)
    for d in range(REP):
        first = pl.multiple_of(((lax.axis_index("rep") + REP - d) % REP) * 512, 512)
        out_ref[:, pl.ds(first, 512)] = pieces[d][:WIDTH, :]
        total = total + dot(pieces[d][WIDTH:, :TILE], packs[d][TILE:, :])
    scratch[...] = total.T
    own = scratch[pl.ds(pl.multiple_of(lax.axis_index("rep") * WIDTH, WIDTH), WIDTH), :]
    virtual_ref[...] = own.T[:G, :].astype(BF16)


def send_rep(values):
    return [values[0]] + [
        lax.ppermute(values[d], "rep", [(i, (i + d) % REP) for i in range(REP)]) for d in range(1, REP)
    ]


def shards(features, virtual_state, w_query, w_key, w_value, w_out, tile_map, local_nbr):
    map_t = tile_map.T

    wanted_from = pl.pallas_call(
        wanted_rows_kernel,
        out_shape=vmem_out((PEERS, TILE), jnp.int32),
        in_specs=[VMEM],
        out_specs=VMEM,
        compiler_params=params(2),
        name="wanted_rows",
    )(in_vmem(map_t))
    wanted = lax.all_to_all(wanted_from.reshape(PEERS, 1, TILE), "nodes", 0, 0, tiled=True)

    rows_in_vmem, pack, virtual_rows, state = pl.pallas_call(
        prepare_kernel,
        out_shape=[
            vmem_out((2048, D), BF16),
            vmem_out((D, D), BF16),
            vmem_out((TILE, D), BF16),
            vmem_out((2 * G, TILE), BF16),
        ],
        in_specs=[pl.BlockSpec(memory_space=pl.ANY)] * 5 + [VMEM],
        out_specs=[VMEM] * 4,
        scratch_shapes=[pltpu.SemaphoreType.DMA((4 + PIECES,))],
        compiler_params=params(16),
        name="prepare",
    )(*map(in_hbm, (features, w_value.T, w_key.T, w_out, w_query.T)), virtual_state)
    packs = [in_vmem(p) for p in send_rep([pack] * REP)]

    own = pl.pallas_call(
        own_part_kernel,
        out_shape=[
            vmem_out((4, 4, 2 * TILE, TILE), BF16),
            vmem_out((4, 4, OWN, 2 * TILE), jnp.float32),
            vmem_out((4, D, 2 * TILE), BF16),
            vmem_out((D, D), BF16),
        ],
        in_specs=[VMEM] * (3 + REP),
        out_specs=[VMEM] * 4,
        compiler_params=params(16),
        name="own_part",
    )(in_vmem(rows_in_vmem), local_nbr.T, in_vmem(virtual_rows), *packs)

    outgoing = pl.pallas_call(
        gather_send_kernel,
        out_shape=vmem_out((PEERS, 8, 9 * TILE), BF16),
        in_specs=[VMEM] * 3,
        out_specs=VMEM,
        compiler_params=params(2),
        name="gather_send",
    )(in_vmem(wanted.reshape(PEERS, TILE)), in_vmem(rows_in_vmem.reshape(PEERS, QUARTER, D)), in_vmem(state))
    arrived = lax.all_to_all(outgoing, "nodes", 0, 0, tiled=True)

    sends = pl.pallas_call(
        gather_rep_kernel,
        out_shape=[vmem_out((4 * len(blocks), QUARTER, D), BF16) for blocks in CHUNKS for _ in range(REP)],
        in_specs=[SMEM] + [VMEM] * REP,
        out_specs=[VMEM] * (len(CHUNKS) * REP),
        compiler_params=params(2),
        name="gather_rep",
    )(map_t, in_vmem(arrived), *packs[1:])
    pieces = [send_rep(sends[k * REP : k * REP + REP]) for k in range(len(CHUNKS))]
    heads = pl.pallas_call(
        join_virtual_kernel,
        out_shape=vmem_out((2 * G, TILE), BF16),
        in_specs=[VMEM],
        out_specs=VMEM,
        compiler_params=params(4),
        name="join_virtual",
    )(in_vmem(arrived))

    rows = None
    for k, blocks in enumerate(CHUNKS):
        last = k == len(CHUNKS) - 1
        args = [*map(in_vmem, (*pieces[k], *own)), *packs]
        args += [in_vmem(heads), in_vmem(rows)] if last else []
        count = len(blocks)
        rows = pl.pallas_call(
            lambda *refs, k=k: attention_kernel(k, *refs),
            out_shape=[vmem_out((WIDTH + 2 * G, 512), BF16)] * REP if last else vmem_out((D, count * TILE), BF16),
            in_specs=[VMEM] * len(args),
            out_specs=[VMEM] * REP if last else VMEM,
            scratch_shapes=[pltpu.VMEM((D, count * TILE), BF16)] * last
            + [
                pltpu.VMEM((count, NEAR, D), BF16),
                pltpu.VMEM((count, D, NEAR), BF16),
                pltpu.VMEM((2, NEAR, 2 * TILE), jnp.float32),
                pltpu.VMEM((2, 2 * TILE + NEAR, 2 * TILE), BF16),
            ],
            compiler_params=params(24),
        )(*args)
    received = send_rep(rows)
    return_shape = [jax.ShapeDtypeStruct((WIDTH, 2048), BF16), jax.ShapeDtypeStruct((G, WIDTH), BF16)]
    node_out, virtual_out = pl.pallas_call(
        assemble_kernel,
        out_shape=return_shape,
        in_specs=[VMEM] * (2 * REP),
        out_specs=[VMEM] * 2,
        scratch_shapes=[pltpu.VMEM((D, 2 * G), jnp.float32)],
        compiler_params=params(4),
        name="assemble",
    )(*map(in_vmem, received), *packs)
    return node_out.T, virtual_out


def solution(mesh):
    in_specs = (
        P("nodes", None),
        P(),
        P(None, "rep"),
        P(None, "rep"),
        P(None, "rep"),
        P("rep", None),
        P("nodes", None),
        P("nodes", None),
    )
    out_specs = (P("nodes", "rep"), P(None, "rep"))
    return jax.shard_map(shards, mesh=mesh, in_specs=in_specs, out_specs=out_specs, check_vma=False)
```

```python
import math

import jax
import jax.numpy as jnp
from jax import lax
from jax.experimental import pallas as pl
from jax.experimental.pallas import tpu as pltpu
from jax.sharding import PartitionSpec as P


D = 256
H = 8
TILE = 128
G = 4
HEAD = D // H
REP = 4
PEERS = 64
WIDTH = D // REP
QUARTER = TILE // REP
SCORE_SCALE = 1.0 / math.sqrt(HEAD)
EXP2_SCALE = SCORE_SCALE * math.log2(math.e)
NEG = -1e30
NT = (((1,), (1,)), ((), ()))
NN = (((1,), (0,)), ((), ()))

SMEM = pl.BlockSpec(memory_space=pltpu.SMEM)
VMEM = pl.BlockSpec(memory_space=pltpu.VMEM)
CHUNKS = ((0, 1), (2, 3))
KEYS = 5 * TILE + 16
PIECES = 4
BF16 = jnp.bfloat16


def dot(a, b, dims=NN, precision=None):
    return lax.dot_general(a, b, dims, precision=precision, preferred_element_type=jnp.float32)


def in_vmem(value):
    return pltpu.with_memory_space_constraint(value, pltpu.VMEM)


def in_hbm(value):
    return pltpu.with_memory_space_constraint(value, pltpu.HBM)


def vmem_out(shape, dtype):
    return pltpu.VMEM(shape, dtype)


def params(mib):
    return pltpu.CompilerParams(vmem_limit_bytes=mib * 1024 * 1024)


def wanted_rows_kernel(map_ref, out_ref):
    blocks = map_ref[...]
    peer = lax.broadcasted_iota(jnp.int32, (PEERS, 16), 0)
    found = jnp.zeros((PEERS, 16), jnp.int32)
    for j in range(4):
        row = blocks[j : j + 1, :]
        found = found + jnp.where(peer == row // 16, row % 16, 0)
    out_ref[...] = jnp.broadcast_to(jnp.sum(found, axis=1, keepdims=True), (PEERS, TILE))


def gather_send_kernel(want_ref, feat_ref, state_ref, out_ref):
    state = state_ref[...]
    for e in range(PEERS):
        rows = feat_ref[want_ref[e : e + 1, :][0, 0] * REP + lax.axis_index("rep")]
        for t in range(8):
            out_ref[e, :, t * TILE : (t + 1) * TILE] = rows[t // 2 * 8 : t // 2 * 8 + 8, t % 2 * TILE : (t % 2 + 1) * TILE]
        out_ref[e, :, 8 * TILE :] = state


def gather_rep_kernel(map_ref, arrived_ref, *refs):
    outs = refs[REP - 1 :]
    for k, blocks in enumerate(CHUNKS):
        for d in range(REP):
            column = ((lax.axis_index("rep") + d) % REP) * 4 + blocks[0]
            for j in range(4 * len(blocks)):
                owner = map_ref[j % 4, column + j // 4] // 16
                for t in range(8):
                    piece = arrived_ref[owner, :, t * TILE : (t + 1) * TILE]
                    outs[k * REP + d][j, t // 2 * 8 : t // 2 * 8 + 8, t % 2 * TILE : (t % 2 + 1) * TILE] = piece


def thirds(value):
    high = value.astype(BF16).astype(jnp.float32)
    middle = (value - high).astype(BF16).astype(jnp.float32)
    return high, middle, value - high - middle


def join_virtual_kernel(arrived_ref, heads_ref):
    parts = arrived_ref[:, :, 8 * TILE :].astype(jnp.float32)
    flat = parts.reshape(PEERS * 2 * G, TILE)
    weighted = (flat + pltpu.roll(flat, TILE - HEAD, 1) + pltpu.roll(flat, TILE - 2 * HEAD, 1)).reshape(parts.shape)
    total = parts[:, :, 96:97] + parts[:, :, 97:98] + parts[:, :, 98:99]
    top = parts[:, :, 99:100] + parts[:, :, 100:101] + parts[:, :, 101:102]
    scale = jnp.exp2((top - jnp.max(top, axis=0, keepdims=True)) * EXP2_SCALE)
    heads = jnp.sum(weighted * scale, axis=0) * (1.0 / jnp.sum(total * scale, axis=0))
    lane = lax.broadcasted_iota(jnp.int32, (2 * G, TILE), 1)
    heads = jnp.where(lane < HEAD, heads, 0.0)
    moved = pltpu.roll(heads, HEAD, 1)
    heads_ref[...] = jnp.concatenate([heads[:G] + moved[G:], jnp.zeros((G, TILE), jnp.float32)], axis=0).astype(BF16)


def prepare_kernel(
    feat_in, value_in, key_in, out_in, query_in, vs_ref, feat_ref, pack_ref, virtual_ref, state_ref, sems
):
    copies = [
        pltpu.make_async_copy(part, pack_ref.at[i * WIDTH : (i + 1) * WIDTH], sems.at[i])
        for i, part in enumerate((value_in, key_in, out_in, query_in))
    ]
    size = 2048 // PIECES
    for i in range(PIECES):
        rows = slice(i * size, (i + 1) * size)
        copies.append(pltpu.make_async_copy(feat_in.at[rows], feat_ref.at[rows], sems.at[4 + i]))
    for copy in copies:
        copy.start()
    vs = vs_ref[...]
    virtual_ref[...] = jnp.concatenate([vs, jnp.zeros((TILE - G, D), BF16)], axis=0)
    for copy in copies[:4]:
        copy.wait()
    q = dot(jnp.concatenate([vs, vs], axis=0), pack_ref[TILE:, :], NT)
    lane = lax.broadcasted_iota(jnp.int32, (2 * G, TILE), 1)
    row = lax.broadcasted_iota(jnp.int32, (2 * G, TILE), 0)
    first = WIDTH + HEAD * (row // G)
    q = jnp.where((lane >= first) & (lane < first + HEAD), q, 0.0).astype(BF16)
    weights = pack_ref[:TILE, :]
    kv, s = [], []
    for i in range(PIECES):
        copies[4 + i].wait()
        kv.append(dot(feat_ref[i * size : (i + 1) * size, :], weights, NT).astype(BF16))
        s.append(dot(q, kv[i], NT))
    s = jnp.concatenate(s, axis=1)
    top = jnp.max(s, axis=1, keepdims=True)
    p = jnp.exp2((s - top) * EXP2_SCALE)
    total = jnp.sum(p, axis=1, keepdims=True)
    w = dot(jnp.concatenate(thirds(p), axis=0).astype(BF16), jnp.concatenate(kv, axis=0))
    w = w[: 2 * G] + w[2 * G : 4 * G] + w[4 * G :]
    w = jnp.where(row < G, w, pltpu.roll(w, TILE - HEAD, 1))
    parts = thirds(w)
    state = jnp.where(lane < HEAD, parts[0], 0.0)
    for i in (1, 2):
        state = jnp.where((lane >= i * HEAD) & (lane < (i + 1) * HEAD), pltpu.roll(parts[i], i * HEAD, 1), state)
    for i, column in enumerate((*thirds(total), *thirds(top))):
        state = jnp.where(lane == 96 + i, column, state)
    state_ref[...] = state.astype(BF16)


def masks_kernel(links_ref, *refs):
    packs, (bias_ref, w_out_ref) = refs[:REP], refs[REP:]
    w_out = jnp.concatenate([p[2 * WIDTH : 3 * WIDTH, :] for p in packs], axis=0)
    w_out_ref[...] = w_out.astype(jnp.float32).T.astype(BF16)
    position = lax.broadcasted_iota(jnp.int32, (TILE, TILE), 0)
    for c in range(4):
        first = pl.multiple_of(lax.axis_index("rep") * 512 + c * TILE, TILE)
        links = links_ref[:, pl.ds(first, TILE)]
        linked = position == links[0:1, :]
        for n in range(1, 16):
            linked = linked | (position == links[n : n + 1, :])
        bias_ref[:, c * TILE : (c + 1) * TILE] = jnp.where(linked, 0.0, NEG)


def attention(blocks, feat_ref, ns, bias_ref, packs, vs_ref, w_out_ref, key_ref, value_ref, score_ref, weight_ref, query_ref):
    lane = lax.broadcasted_iota(jnp.int32, (TILE, TILE), 1)
    row = lax.broadcasted_iota(jnp.int32, (16, 2 * TILE), 0)
    w_value = jnp.concatenate([p[:WIDTH, :] for p in packs], axis=0)
    w_key = jnp.concatenate([p[WIDTH : 2 * WIDTH, :] for p in packs], axis=0)
    w_query = jnp.concatenate([p[3 * WIDTH :, :] for p in packs], axis=0)
    for b in range(2):
        weight_ref[b, KEYS:, :] = jnp.zeros((6 * TILE - KEYS, 2 * TILE), BF16)

    def project(i):
        first = pl.multiple_of(lax.axis_index("rep") * 512 + blocks[i] * TILE, TILE)
        own = feat_ref[pl.ds(first, TILE), :]
        near = [n[4 * i : 4 * i + 4].reshape(TILE, D) for n in ns]
        key_ref[i] = dot(jnp.concatenate([own, *near, vs_ref[:16, :]], axis=0), w_key, NT).astype(BF16)
        value_ref[i] = dot(w_value, jnp.concatenate([own, *near, vs_ref[...]], axis=0), NT).astype(BF16)
        q = dot(own, w_query, NT)
        for pair in range(4):
            part = q[:, pair // 2 * TILE : (pair // 2 + 1) * TILE]
            for k in range(2):
                low = (2 * pair + k) % 4 * HEAD
                masked = jnp.where((lane >= low) & (lane < low + HEAD), part, 0.0).astype(BF16)
                query_ref[i, pair, k * TILE : (k + 1) * TILE, :] = masked

    def score(n):
        i, pair = divmod(n, 4)
        s = dot(key_ref[i, :, pair // 2 * TILE : (pair // 2 + 1) * TILE], query_ref[i, pair], NT)
        bias = bias_ref[:, blocks[i] * TILE : (blocks[i] + 1) * TILE]
        bias = jnp.concatenate([bias, bias], axis=1)
        near, far = s[:TILE] + bias, jnp.where(row < G, s[5 * TILE :], NEG)
        score_ref[n % 2] = jnp.concatenate([near, s[TILE : 5 * TILE], far], axis=0)

    def weigh(n):
        s = score_ref[n % 2]
        p = jnp.exp2((s - jnp.max(s, axis=0, keepdims=True)) * EXP2_SCALE)
        weight_ref[n % 2, :KEYS, :] = p.astype(BF16)
        return 1.0 / jnp.sum(p, axis=0, keepdims=True)

    def blend(n, scale):
        i, pair = divmod(n, 4)
        o = dot(value_ref[i, pair * WIDTH : (pair + 1) * WIDTH, :], weight_ref[n % 2]) * scale
        return jnp.concatenate([o[:HEAD, :TILE], o[HEAD:, TILE:]], axis=0)

    project(0)
    score(0)
    parts, scale = [], None
    for n in range(4 * len(blocks)):
        if n % 4 == 1 and n // 4 + 1 < len(blocks):
            project(n // 4 + 1)
        if n + 1 < 4 * len(blocks):
            score(n + 1)
        if n:
            parts.append(blend(n - 1, scale))
        scale = weigh(n)
    parts.append(blend(4 * len(blocks) - 1, scale))
    heads = [jnp.concatenate(parts[4 * i : 4 * i + 4], axis=0) for i in range(len(blocks))]
    return dot(w_out_ref[...], jnp.concatenate(heads, axis=1).astype(BF16)).astype(BF16)


def attention_kernel(chunk, feat_ref, *refs):
    ns, refs = refs[:REP], refs[REP:]
    bias_ref, refs = refs[0], refs[1:]
    packs, refs = refs[:REP], refs[REP:]
    (vs_ref, w_out_ref), refs = refs[:2], refs[2:]
    refs, scratch = refs[:-5], refs[-5:]
    out = attention(CHUNKS[chunk], feat_ref, ns, bias_ref, packs, vs_ref, w_out_ref, *scratch)
    if chunk == 0:
        refs[0][...] = out
        return
    heads_ref, before_ref, *outs, own_ref = refs
    own_ref[...] = out
    done = before_ref.shape[1]
    for d in range(REP):
        first = pl.multiple_of(((lax.axis_index("rep") + d) % REP) * WIDTH, WIDTH)
        outs[d][:WIDTH, :done] = before_ref[pl.ds(first, WIDTH), :]
        outs[d][:WIDTH, done:] = own_ref[pl.ds(first, WIDTH), :]
        outs[d][WIDTH:, :TILE] = heads_ref[...]
        outs[d][WIDTH:, TILE:] = jnp.zeros((2 * G, 3 * TILE), BF16)


def assemble_kernel(*refs):
    pieces, packs, (out_ref, virtual_ref, scratch) = refs[:REP], refs[REP : 2 * REP], refs[2 * REP :]
    total = jnp.zeros((2 * G, D), jnp.float32)
    for d in range(REP):
        first = pl.multiple_of(((lax.axis_index("rep") + REP - d) % REP) * 512, 512)
        out_ref[:, pl.ds(first, 512)] = pieces[d][:WIDTH, :]
        total = total + dot(pieces[d][WIDTH:, :TILE], packs[d][TILE:, :])
    scratch[...] = total.T
    own = scratch[pl.ds(pl.multiple_of(lax.axis_index("rep") * WIDTH, WIDTH), WIDTH), :]
    virtual_ref[...] = own.T[:G, :].astype(BF16)


def send_rep(values):
    received = list(values)
    for d in (1, 3, 2):
        received[d] = lax.ppermute(values[d], "rep", [(i, (i + d) % REP) for i in range(REP)])
    return received


def shards(features, virtual_state, w_query, w_key, w_value, w_out, tile_map, local_nbr):
    map_t = tile_map.T

    wanted_from = pl.pallas_call(
        wanted_rows_kernel,
        out_shape=vmem_out((PEERS, TILE), jnp.int32),
        in_specs=[VMEM],
        out_specs=VMEM,
        compiler_params=params(2),
        name="wanted_rows",
    )(in_vmem(map_t))
    wanted = lax.all_to_all(wanted_from.reshape(PEERS, 1, TILE), "nodes", 0, 0, tiled=True)

    rows_in_vmem, pack, virtual_rows, state = pl.pallas_call(
        prepare_kernel,
        out_shape=[
            vmem_out((2048, D), BF16),
            vmem_out((D, D), BF16),
            vmem_out((TILE, D), BF16),
            vmem_out((2 * G, TILE), BF16),
        ],
        in_specs=[pl.BlockSpec(memory_space=pl.ANY)] * 5 + [VMEM],
        out_specs=[VMEM] * 4,
        scratch_shapes=[pltpu.SemaphoreType.DMA((4 + PIECES,))],
        compiler_params=params(16),
        name="prepare",
    )(*map(in_hbm, (features, w_value.T, w_key.T, w_out, w_query.T)), virtual_state)
    packs = [in_vmem(p) for p in send_rep([pack] * REP)]

    bias, w_out_t = pl.pallas_call(
        masks_kernel,
        out_shape=[vmem_out((TILE, 512), jnp.float32), vmem_out((D, D), BF16)],
        in_specs=[VMEM] * (1 + REP),
        out_specs=[VMEM] * 2,
        compiler_params=params(2),
        name="masks",
    )(local_nbr.T, *packs)

    outgoing = pl.pallas_call(
        gather_send_kernel,
        out_shape=vmem_out((PEERS, 8, 9 * TILE), BF16),
        in_specs=[VMEM] * 3,
        out_specs=VMEM,
        compiler_params=params(2),
        name="gather_send",
    )(in_vmem(wanted.reshape(PEERS, TILE)), in_vmem(rows_in_vmem.reshape(PEERS, QUARTER, D)), in_vmem(state))
    arrived = lax.all_to_all(outgoing, "nodes", 0, 0, tiled=True)

    sends = pl.pallas_call(
        gather_rep_kernel,
        out_shape=[vmem_out((4 * len(blocks), QUARTER, D), BF16) for blocks in CHUNKS for _ in range(REP)],
        in_specs=[SMEM] + [VMEM] * REP,
        out_specs=[VMEM] * (len(CHUNKS) * REP),
        compiler_params=params(2),
        name="gather_rep",
    )(map_t, in_vmem(arrived), *packs[1:])
    pieces = [send_rep(sends[k * REP : k * REP + REP]) for k in range(len(CHUNKS))]
    heads = pl.pallas_call(
        join_virtual_kernel,
        out_shape=vmem_out((2 * G, TILE), BF16),
        in_specs=[VMEM],
        out_specs=VMEM,
        compiler_params=params(4),
        name="join_virtual",
    )(in_vmem(arrived))

    rows = None
    for k, blocks in enumerate(CHUNKS):
        last = k == len(CHUNKS) - 1
        args = [in_vmem(rows_in_vmem), *map(in_vmem, pieces[k]), in_vmem(bias), *packs, in_vmem(virtual_rows), in_vmem(w_out_t)]
        args += [in_vmem(heads), in_vmem(rows)] if last else []
        count = len(blocks)
        rows = pl.pallas_call(
            lambda *refs, k=k: attention_kernel(k, *refs),
            out_shape=[vmem_out((WIDTH + 2 * G, 512), BF16)] * REP if last else vmem_out((D, count * TILE), BF16),
            in_specs=[VMEM] * len(args),
            out_specs=[VMEM] * REP if last else VMEM,
            scratch_shapes=[pltpu.VMEM((D, count * TILE), BF16)] * last
            + [
                pltpu.VMEM((count, KEYS, D), BF16),
                pltpu.VMEM((count, D, 6 * TILE), BF16),
                pltpu.VMEM((2, KEYS, 2 * TILE), jnp.float32),
                pltpu.VMEM((2, 6 * TILE, 2 * TILE), BF16),
                pltpu.VMEM((count, 4, 2 * TILE, TILE), BF16),
            ],
            compiler_params=params(24),
        )(*args)
    received = send_rep(rows)
    return_shape = [jax.ShapeDtypeStruct((WIDTH, 2048), BF16), jax.ShapeDtypeStruct((G, WIDTH), BF16)]
    node_out, virtual_out = pl.pallas_call(
        assemble_kernel,
        out_shape=return_shape,
        in_specs=[VMEM] * (2 * REP),
        out_specs=[VMEM] * 2,
        scratch_shapes=[pltpu.VMEM((D, 2 * G), jnp.float32)],
        compiler_params=params(4),
        name="assemble",
    )(*map(in_vmem, received), *packs)
    return node_out.T, virtual_out


def solution(mesh):
    in_specs = (
        P("nodes", None),
        P(),
        P(None, "rep"),
        P(None, "rep"),
        P(None, "rep"),
        P("rep", None),
        P("nodes", None),
        P("nodes", None),
    )
    out_specs = (P("nodes", "rep"), P(None, "rep"))
    return jax.shard_map(shards, mesh=mesh, in_specs=in_specs, out_specs=out_specs, check_vma=False)
```

```python
import math

import jax
import jax.numpy as jnp
from jax import lax
from jax.experimental import pallas as pl
from jax.experimental.pallas import tpu as pltpu
from jax.sharding import PartitionSpec as P


D = 256
H = 8
TILE = 128
G = 4
HEAD = D // H
REP = 4
PEERS = 64
WIDTH = D // REP
QUARTER = TILE // REP
SCORE_SCALE = 1.0 / math.sqrt(HEAD)
EXP2_SCALE = SCORE_SCALE * math.log2(math.e)
NEG = -1e30
NT = (((1,), (1,)), ((), ()))
NN = (((1,), (0,)), ((), ()))

SMEM = pl.BlockSpec(memory_space=pltpu.SMEM)
VMEM = pl.BlockSpec(memory_space=pltpu.VMEM)
CHUNKS = ((0, 1), (2, 3))
KEYS = 5 * TILE + 16
PIECES = 4
BF16 = jnp.bfloat16


def dot(a, b, dims=NN, precision=None):
    return lax.dot_general(a, b, dims, precision=precision, preferred_element_type=jnp.float32)


def in_vmem(value):
    return pltpu.with_memory_space_constraint(value, pltpu.VMEM)


def in_hbm(value):
    return pltpu.with_memory_space_constraint(value, pltpu.HBM)


def vmem_out(shape, dtype):
    return pltpu.VMEM(shape, dtype)


def params(mib):
    return pltpu.CompilerParams(vmem_limit_bytes=mib * 1024 * 1024)


def wanted_rows_kernel(map_ref, out_ref):
    blocks = map_ref[...]
    peer = lax.broadcasted_iota(jnp.int32, (PEERS, 16), 0)
    found = jnp.zeros((PEERS, 16), jnp.int32)
    for j in range(4):
        row = blocks[j : j + 1, :]
        found = found + jnp.where(peer == row // 16, row % 16, 0)
    out_ref[...] = jnp.broadcast_to(jnp.sum(found, axis=1, keepdims=True), (PEERS, TILE))


def gather_send_kernel(want_ref, feat_ref, state_ref, out_ref, slots_ref, sems):
    state = state_ref[...]
    size = PEERS // PIECES
    copies = []
    for i in range(PIECES):
        for e in range(i * size, (i + 1) * size):
            rows = feat_ref[want_ref[e : e + 1, :][0, 0] * REP + lax.axis_index("rep")]
            for t in range(8):
                part = rows[t // 2 * 8 : t // 2 * 8 + 8, t % 2 * TILE : (t % 2 + 1) * TILE]
                slots_ref[e, :, t * TILE : (t + 1) * TILE] = part
            slots_ref[e, :, 8 * TILE :] = state
        part = slice(i * size, (i + 1) * size)
        copies.append(pltpu.make_async_copy(slots_ref.at[part], out_ref.at[part], sems.at[i]))
        copies[i].start()
    for copy in copies:
        copy.wait()


def gather_rep_kernel(blocks, owner_ref, arrived_ref, *outs):
    for d in range(REP):
        for j in range(4 * len(blocks)):
            owner = owner_ref[d * 16 + 4 * blocks[0] + j][0, 0]
            for t in range(8):
                piece = arrived_ref[owner, :, t * TILE : (t + 1) * TILE]
                outs[d][j, t // 2 * 8 : t // 2 * 8 + 8, t % 2 * TILE : (t % 2 + 1) * TILE] = piece


def thirds(value):
    high = value.astype(BF16).astype(jnp.float32)
    middle = (value - high).astype(BF16).astype(jnp.float32)
    return high, middle, value - high - middle


def join_virtual_kernel(arrived_ref, heads_ref):
    parts = arrived_ref[:, :, 8 * TILE :].astype(jnp.float32)
    flat = parts.reshape(PEERS * 2 * G, TILE)
    weighted = (flat + pltpu.roll(flat, TILE - HEAD, 1) + pltpu.roll(flat, TILE - 2 * HEAD, 1)).reshape(parts.shape)
    total = parts[:, :, 96:97] + parts[:, :, 97:98] + parts[:, :, 98:99]
    top = parts[:, :, 99:100] + parts[:, :, 100:101] + parts[:, :, 101:102]
    scale = jnp.exp2((top - jnp.max(top, axis=0, keepdims=True)) * EXP2_SCALE)
    heads = jnp.sum(weighted * scale, axis=0) * (1.0 / jnp.sum(total * scale, axis=0))
    lane = lax.broadcasted_iota(jnp.int32, (2 * G, TILE), 1)
    heads = jnp.where(lane < HEAD, heads, 0.0)
    moved = pltpu.roll(heads, HEAD, 1)
    heads_ref[...] = jnp.concatenate([heads[:G] + moved[G:], jnp.zeros((G, TILE), jnp.float32)], axis=0).astype(BF16)


def prepare_kernel(
    feat_in, value_in, key_in, out_in, query_in, vs_ref, feat_ref, pack_ref, virtual_ref, state_ref, sems
):
    copies = [
        pltpu.make_async_copy(part, pack_ref.at[i * WIDTH : (i + 1) * WIDTH], sems.at[i])
        for i, part in enumerate((value_in, key_in, out_in, query_in))
    ]
    size = 2048 // PIECES
    for i in range(PIECES):
        rows = slice(i * size, (i + 1) * size)
        copies.append(pltpu.make_async_copy(feat_in.at[rows], feat_ref.at[rows], sems.at[4 + i]))
    for copy in copies:
        copy.start()
    vs = vs_ref[...]
    virtual_ref[...] = jnp.concatenate([vs, jnp.zeros((TILE - G, D), BF16)], axis=0)
    for copy in copies[:4]:
        copy.wait()
    q = dot(jnp.concatenate([vs, vs], axis=0), pack_ref[TILE:, :], NT)
    lane = lax.broadcasted_iota(jnp.int32, (2 * G, TILE), 1)
    row = lax.broadcasted_iota(jnp.int32, (2 * G, TILE), 0)
    first = WIDTH + HEAD * (row // G)
    q = jnp.where((lane >= first) & (lane < first + HEAD), q, 0.0).astype(BF16)
    weights = pack_ref[:TILE, :]
    kv, s = [], []
    for i in range(PIECES):
        copies[4 + i].wait()
        kv.append(dot(feat_ref[i * size : (i + 1) * size, :], weights, NT).astype(BF16))
        s.append(dot(q, kv[i], NT))
    s = jnp.concatenate(s, axis=1)
    top = jnp.max(s, axis=1, keepdims=True)
    p = jnp.exp2((s - top) * EXP2_SCALE)
    total = jnp.sum(p, axis=1, keepdims=True)
    w = dot(jnp.concatenate(thirds(p), axis=0).astype(BF16), jnp.concatenate(kv, axis=0))
    w = w[: 2 * G] + w[2 * G : 4 * G] + w[4 * G :]
    w = jnp.where(row < G, w, pltpu.roll(w, TILE - HEAD, 1))
    parts = thirds(w)
    state = jnp.where(lane < HEAD, parts[0], 0.0)
    for i in (1, 2):
        state = jnp.where((lane >= i * HEAD) & (lane < (i + 1) * HEAD), pltpu.roll(parts[i], i * HEAD, 1), state)
    for i, column in enumerate((*thirds(total), *thirds(top))):
        state = jnp.where(lane == 96 + i, column, state)
    state_ref[...] = state.astype(BF16)


def masks_kernel(links_ref, map_ref, *refs):
    packs, (bias_ref, w_out_ref, owner_ref) = refs[:REP], refs[REP:]
    owners = map_ref[...] // 16
    for plane in range(REP):
        first = (plane + REP - lax.axis_index("rep")) % REP * 16
        for j in range(16):
            column = 4 * plane + j // 4
            owner = owners[j % 4 : j % 4 + 1, column : column + 1]
            owner_ref[first + j] = jnp.broadcast_to(owner, (1, TILE))
    w_out = jnp.concatenate([p[2 * WIDTH : 3 * WIDTH, :] for p in packs], axis=0)
    w_out_ref[...] = w_out.astype(jnp.float32).T.astype(BF16)
    position = lax.broadcasted_iota(jnp.int32, (TILE, TILE), 0)
    for c in range(4):
        first = pl.multiple_of(lax.axis_index("rep") * 512 + c * TILE, TILE)
        links = links_ref[:, pl.ds(first, TILE)]
        linked = position == links[0:1, :]
        for n in range(1, 16):
            linked = linked | (position == links[n : n + 1, :])
        bias_ref[:, c * TILE : (c + 1) * TILE] = jnp.where(linked, 0.0, NEG)


def attention(blocks, feat_ref, ns, bias_ref, packs, vs_ref, w_out_ref, key_ref, value_ref, score_ref, weight_ref, query_ref):
    lane = lax.broadcasted_iota(jnp.int32, (TILE, TILE), 1)
    row = lax.broadcasted_iota(jnp.int32, (16, 2 * TILE), 0)
    w_value = jnp.concatenate([p[:WIDTH, :] for p in packs], axis=0)
    w_key = jnp.concatenate([p[WIDTH : 2 * WIDTH, :] for p in packs], axis=0)
    w_query = jnp.concatenate([p[3 * WIDTH :, :] for p in packs], axis=0)
    for b in range(2):
        weight_ref[b, KEYS:, :] = jnp.zeros((6 * TILE - KEYS, 2 * TILE), BF16)

    def project(i):
        first = pl.multiple_of(lax.axis_index("rep") * 512 + blocks[i] * TILE, TILE)
        own = feat_ref[pl.ds(first, TILE), :]
        near = [n[4 * i : 4 * i + 4].reshape(TILE, D) for n in ns]
        key_ref[i] = dot(jnp.concatenate([own, *near, vs_ref[:16, :]], axis=0), w_key, NT).astype(BF16)
        value_ref[i] = dot(w_value, jnp.concatenate([own, *near, vs_ref[...]], axis=0), NT).astype(BF16)
        q = dot(own, w_query, NT)
        for pair in range(4):
            part = q[:, pair // 2 * TILE : (pair // 2 + 1) * TILE]
            for k in range(2):
                low = (2 * pair + k) % 4 * HEAD
                masked = jnp.where((lane >= low) & (lane < low + HEAD), part, 0.0).astype(BF16)
                query_ref[i, pair, k * TILE : (k + 1) * TILE, :] = masked

    def score(n):
        i, pair = divmod(n, 4)
        s = dot(key_ref[i, :, pair // 2 * TILE : (pair // 2 + 1) * TILE], query_ref[i, pair], NT)
        bias = bias_ref[:, blocks[i] * TILE : (blocks[i] + 1) * TILE]
        bias = jnp.concatenate([bias, bias], axis=1)
        near, far = s[:TILE] + bias, jnp.where(row < G, s[5 * TILE :], NEG)
        score_ref[n % 2] = jnp.concatenate([near, s[TILE : 5 * TILE], far], axis=0)

    def weigh(n):
        s = score_ref[n % 2]
        p = jnp.exp2((s - jnp.max(s, axis=0, keepdims=True)) * EXP2_SCALE)
        weight_ref[n % 2, :KEYS, :] = p.astype(BF16)
        return 1.0 / jnp.sum(p, axis=0, keepdims=True)

    def blend(n, scale):
        i, pair = divmod(n, 4)
        o = dot(value_ref[i, pair * WIDTH : (pair + 1) * WIDTH, :], weight_ref[n % 2]) * scale
        return jnp.concatenate([o[:HEAD, :TILE], o[HEAD:, TILE:]], axis=0)

    project(0)
    score(0)
    parts, scale = [], None
    for n in range(4 * len(blocks)):
        if n % 4 == 1 and n // 4 + 1 < len(blocks):
            project(n // 4 + 1)
        if n + 1 < 4 * len(blocks):
            score(n + 1)
        if n:
            parts.append(blend(n - 1, scale))
        scale = weigh(n)
    parts.append(blend(4 * len(blocks) - 1, scale))
    heads = [jnp.concatenate(parts[4 * i : 4 * i + 4], axis=0) for i in range(len(blocks))]
    return dot(w_out_ref[...], jnp.concatenate(heads, axis=1).astype(BF16)).astype(BF16)


def attention_kernel(chunk, feat_ref, *refs):
    ns, refs = refs[:REP], refs[REP:]
    bias_ref, refs = refs[0], refs[1:]
    packs, refs = refs[:REP], refs[REP:]
    (vs_ref, w_out_ref), refs = refs[:2], refs[2:]
    refs, scratch = refs[:-5], refs[-5:]
    out = attention(CHUNKS[chunk], feat_ref, ns, bias_ref, packs, vs_ref, w_out_ref, *scratch)
    if chunk == 0:
        refs[0][...] = out
        return
    heads_ref, before_ref, *outs, own_ref = refs
    own_ref[...] = out
    done = before_ref.shape[1]
    for d in range(REP):
        first = pl.multiple_of(((lax.axis_index("rep") + d) % REP) * WIDTH, WIDTH)
        outs[d][:WIDTH, :done] = before_ref[pl.ds(first, WIDTH), :]
        outs[d][:WIDTH, done:] = own_ref[pl.ds(first, WIDTH), :]
        outs[d][WIDTH:, :TILE] = heads_ref[...]
        outs[d][WIDTH:, TILE:] = jnp.zeros((2 * G, 3 * TILE), BF16)


def assemble_kernel(*refs):
    pieces, packs, (out_ref, virtual_ref, scratch, sems) = refs[:REP], refs[REP : 2 * REP], refs[2 * REP :]
    copies = []
    for d in range(REP):
        first = pl.multiple_of(((lax.axis_index("rep") + REP - d) % REP) * 512, 512)
        copies.append(pltpu.make_async_copy(pieces[d].at[:WIDTH], out_ref.at[:, pl.ds(first, 512)], sems.at[d]))
        copies[d].start()
    total = jnp.zeros((2 * G, D), jnp.float32)
    for d in range(REP):
        total = total + dot(pieces[d][WIDTH:, :TILE], packs[d][TILE:, :])
    scratch[...] = total.T
    own = scratch[pl.ds(pl.multiple_of(lax.axis_index("rep") * WIDTH, WIDTH), WIDTH), :]
    virtual_ref[...] = own.T[:G, :].astype(BF16)
    for copy in copies:
        copy.wait()


def send_rep(values):
    received = list(values)
    for d in (1, 3, 2):
        received[d] = lax.ppermute(values[d], "rep", [(i, (i + d) % REP) for i in range(REP)])
    return received


def shards(features, virtual_state, w_query, w_key, w_value, w_out, tile_map, local_nbr):
    map_t = tile_map.T

    wanted_from = pl.pallas_call(
        wanted_rows_kernel,
        out_shape=vmem_out((PEERS, TILE), jnp.int32),
        in_specs=[VMEM],
        out_specs=VMEM,
        compiler_params=params(2),
        name="wanted_rows",
    )(in_vmem(map_t))
    wanted = lax.all_to_all(wanted_from.reshape(PEERS, 1, TILE), "nodes", 0, 0, tiled=True)

    rows_in_vmem, pack, virtual_rows, state = pl.pallas_call(
        prepare_kernel,
        out_shape=[
            vmem_out((2048, D), BF16),
            vmem_out((D, D), BF16),
            vmem_out((TILE, D), BF16),
            vmem_out((2 * G, TILE), BF16),
        ],
        in_specs=[pl.BlockSpec(memory_space=pl.ANY)] * 5 + [VMEM],
        out_specs=[VMEM] * 4,
        scratch_shapes=[pltpu.SemaphoreType.DMA((4 + PIECES,))],
        compiler_params=params(16),
        name="prepare",
    )(*map(in_hbm, (features, w_value.T, w_key.T, w_out, w_query.T)), virtual_state)
    packs = [in_vmem(p) for p in send_rep([pack] * REP)]

    bias, w_out_t, owners = pl.pallas_call(
        masks_kernel,
        out_shape=[
            vmem_out((TILE, 512), jnp.float32),
            vmem_out((D, D), BF16),
            vmem_out((PEERS, 1, TILE), jnp.int32),
        ],
        in_specs=[VMEM] * (2 + REP),
        out_specs=[VMEM] * 3,
        compiler_params=params(2),
        name="masks",
    )(local_nbr.T, map_t, *packs)

    outgoing = pl.pallas_call(
        gather_send_kernel,
        out_shape=jax.ShapeDtypeStruct((PEERS, 8, 9 * TILE), BF16),
        in_specs=[VMEM] * 3,
        out_specs=pl.BlockSpec(memory_space=pl.ANY),
        scratch_shapes=[pltpu.VMEM((PEERS, 8, 9 * TILE), BF16), pltpu.SemaphoreType.DMA((PIECES,))],
        compiler_params=params(4),
        name="gather_send",
    )(in_vmem(wanted.reshape(PEERS, TILE)), in_vmem(rows_in_vmem.reshape(PEERS, QUARTER, D)), in_vmem(state))
    arrived = lax.all_to_all(outgoing, "nodes", 0, 0, tiled=True)

    pieces = []
    for blocks in CHUNKS:
        sends = pl.pallas_call(
            lambda *refs, blocks=blocks: gather_rep_kernel(blocks, *refs),
            out_shape=[vmem_out((4 * len(blocks), QUARTER, D), BF16)] * REP,
            in_specs=[VMEM] * 2,
            out_specs=[VMEM] * REP,
            compiler_params=params(2),
        )(in_vmem(owners), in_vmem(arrived))
        pieces.append(send_rep(sends))
    heads = pl.pallas_call(
        join_virtual_kernel,
        out_shape=vmem_out((2 * G, TILE), BF16),
        in_specs=[VMEM],
        out_specs=VMEM,
        compiler_params=params(4),
        name="join_virtual",
    )(in_vmem(arrived))

    rows = None
    for k, blocks in enumerate(CHUNKS):
        last = k == len(CHUNKS) - 1
        args = [in_vmem(rows_in_vmem), *map(in_vmem, pieces[k]), in_vmem(bias), *packs, in_vmem(virtual_rows), in_vmem(w_out_t)]
        args += [in_vmem(heads), in_vmem(rows)] if last else []
        count = len(blocks)
        rows = pl.pallas_call(
            lambda *refs, k=k: attention_kernel(k, *refs),
            out_shape=[vmem_out((WIDTH + 2 * G, 512), BF16)] * REP if last else vmem_out((D, count * TILE), BF16),
            in_specs=[VMEM] * len(args),
            out_specs=[VMEM] * REP if last else VMEM,
            scratch_shapes=[pltpu.VMEM((D, count * TILE), BF16)] * last
            + [
                pltpu.VMEM((count, KEYS, D), BF16),
                pltpu.VMEM((count, D, 6 * TILE), BF16),
                pltpu.VMEM((2, KEYS, 2 * TILE), jnp.float32),
                pltpu.VMEM((2, 6 * TILE, 2 * TILE), BF16),
                pltpu.VMEM((count, 4, 2 * TILE, TILE), BF16),
            ],
            compiler_params=params(24),
        )(*args)
    received = send_rep(rows)
    return_shape = [jax.ShapeDtypeStruct((WIDTH, 2048), BF16), jax.ShapeDtypeStruct((G, WIDTH), BF16)]
    node_out, virtual_out = pl.pallas_call(
        assemble_kernel,
        out_shape=return_shape,
        in_specs=[VMEM] * (2 * REP),
        out_specs=[pl.BlockSpec(memory_space=pl.ANY), VMEM],
        scratch_shapes=[pltpu.VMEM((D, 2 * G), jnp.float32), pltpu.SemaphoreType.DMA((REP,))],
        compiler_params=params(4),
        name="assemble",
    )(*map(in_vmem, received), *packs)
    return node_out.T, virtual_out


def solution(mesh):
    in_specs = (
        P("nodes", None),
        P(),
        P(None, "rep"),
        P(None, "rep"),
        P(None, "rep"),
        P("rep", None),
        P("nodes", None),
        P("nodes", None),
    )
    out_specs = (P("nodes", "rep"), P(None, "rep"))
    return jax.shard_map(shards, mesh=mesh, in_specs=in_specs, out_specs=out_specs, check_vma=False)
```

```python
import math

import jax
import jax.numpy as jnp
from jax import lax
from jax.experimental import pallas as pl
from jax.experimental.pallas import tpu as pltpu
from jax.sharding import PartitionSpec as P


D = 256
H = 8
TILE = 128
G = 4
HEAD = D // H
REP = 4
PEERS = 64
WIDTH = D // REP
QUARTER = TILE // REP
SCORE_SCALE = 1.0 / math.sqrt(HEAD)
EXP2_SCALE = SCORE_SCALE * math.log2(math.e)
NEG = -1e30
NT = (((1,), (1,)), ((), ()))
NN = (((1,), (0,)), ((), ()))

SMEM = pl.BlockSpec(memory_space=pltpu.SMEM)
VMEM = pl.BlockSpec(memory_space=pltpu.VMEM)
CHUNKS = ((0, 1), (2, 3))
KEYS = 5 * TILE + 16
HERE = 2 * TILE + 16
PIECES = 4
BF16 = jnp.bfloat16


def dot(a, b, dims=NN, precision=None):
    return lax.dot_general(a, b, dims, precision=precision, preferred_element_type=jnp.float32)


def in_vmem(value):
    return pltpu.with_memory_space_constraint(value, pltpu.VMEM)


def in_hbm(value):
    return pltpu.with_memory_space_constraint(value, pltpu.HBM)


def vmem_out(shape, dtype):
    return pltpu.VMEM(shape, dtype)


def params(mib):
    return pltpu.CompilerParams(vmem_limit_bytes=mib * 1024 * 1024)


def wanted_rows_kernel(map_ref, out_ref):
    blocks = map_ref[...]
    peer = lax.broadcasted_iota(jnp.int32, (PEERS, 16), 0)
    found = jnp.zeros((PEERS, 16), jnp.int32)
    for j in range(4):
        row = blocks[j : j + 1, :]
        found = found + jnp.where(peer == row // 16, row % 16, 0)
    out_ref[...] = jnp.broadcast_to(jnp.sum(found, axis=1, keepdims=True), (PEERS, TILE))


def gather_send_kernel(want_ref, feat_ref, state_ref, out_ref, slots_ref, sems):
    state = state_ref[...]
    size = PEERS // PIECES
    copies = []
    for i in range(PIECES):
        for e in range(i * size, (i + 1) * size):
            rows = feat_ref[want_ref[e : e + 1, :][0, 0] * REP + lax.axis_index("rep")]
            for t in range(8):
                part = rows[t // 2 * 8 : t // 2 * 8 + 8, t % 2 * TILE : (t % 2 + 1) * TILE]
                slots_ref[e, :, t * TILE : (t + 1) * TILE] = part
            slots_ref[e, :, 8 * TILE :] = state
        part = slice(i * size, (i + 1) * size)
        copies.append(pltpu.make_async_copy(slots_ref.at[part], out_ref.at[part], sems.at[i]))
        copies[i].start()
    for copy in copies:
        copy.wait()


def gather_rep_kernel(blocks, owner_ref, arrived_ref, *outs):
    for d in range(REP):
        for j in range(4 * len(blocks)):
            owner = owner_ref[d * 16 + 4 * blocks[0] + j][0, 0]
            for t in range(8):
                piece = arrived_ref[owner, :, t * TILE : (t + 1) * TILE]
                outs[d][j, t // 2 * 8 : t // 2 * 8 + 8, t % 2 * TILE : (t % 2 + 1) * TILE] = piece


def thirds(value):
    high = value.astype(BF16).astype(jnp.float32)
    middle = (value - high).astype(BF16).astype(jnp.float32)
    return high, middle, value - high - middle


def join_virtual_kernel(arrived_ref, heads_ref):
    parts = arrived_ref[:, :, 8 * TILE :].astype(jnp.float32)
    flat = parts.reshape(PEERS * 2 * G, TILE)
    weighted = (flat + pltpu.roll(flat, TILE - HEAD, 1) + pltpu.roll(flat, TILE - 2 * HEAD, 1)).reshape(parts.shape)
    total = parts[:, :, 96:97] + parts[:, :, 97:98] + parts[:, :, 98:99]
    top = parts[:, :, 99:100] + parts[:, :, 100:101] + parts[:, :, 101:102]
    scale = jnp.exp2((top - jnp.max(top, axis=0, keepdims=True)) * EXP2_SCALE)
    heads = jnp.sum(weighted * scale, axis=0) * (1.0 / jnp.sum(total * scale, axis=0))
    lane = lax.broadcasted_iota(jnp.int32, (2 * G, TILE), 1)
    heads = jnp.where(lane < HEAD, heads, 0.0)
    moved = pltpu.roll(heads, HEAD, 1)
    heads_ref[...] = jnp.concatenate([heads[:G] + moved[G:], jnp.zeros((G, TILE), jnp.float32)], axis=0).astype(BF16)


def prepare_kernel(
    feat_in, value_in, key_in, out_in, query_in, vs_ref, feat_ref, pack_ref, virtual_ref, state_ref, sems
):
    copies = [
        pltpu.make_async_copy(part, pack_ref.at[i * WIDTH : (i + 1) * WIDTH], sems.at[i])
        for i, part in enumerate((value_in, key_in, out_in, query_in))
    ]
    size = 2048 // PIECES
    for i in range(PIECES):
        rows = slice(i * size, (i + 1) * size)
        copies.append(pltpu.make_async_copy(feat_in.at[rows], feat_ref.at[rows], sems.at[4 + i]))
    for copy in copies:
        copy.start()
    vs = vs_ref[...]
    virtual_ref[...] = jnp.concatenate([vs, jnp.zeros((TILE - G, D), BF16)], axis=0)
    for copy in copies[:4]:
        copy.wait()
    q = dot(jnp.concatenate([vs, vs], axis=0), pack_ref[TILE:, :], NT)
    lane = lax.broadcasted_iota(jnp.int32, (2 * G, TILE), 1)
    row = lax.broadcasted_iota(jnp.int32, (2 * G, TILE), 0)
    first = WIDTH + HEAD * (row // G)
    q = jnp.where((lane >= first) & (lane < first + HEAD), q, 0.0).astype(BF16)
    weights = pack_ref[:TILE, :]
    kv, s = [], []
    for i in range(PIECES):
        copies[4 + i].wait()
        kv.append(dot(feat_ref[i * size : (i + 1) * size, :], weights, NT).astype(BF16))
        s.append(dot(q, kv[i], NT))
    s = jnp.concatenate(s, axis=1)
    top = jnp.max(s, axis=1, keepdims=True)
    p = jnp.exp2((s - top) * EXP2_SCALE)
    total = jnp.sum(p, axis=1, keepdims=True)
    w = dot(jnp.concatenate(thirds(p), axis=0).astype(BF16), jnp.concatenate(kv, axis=0))
    w = w[: 2 * G] + w[2 * G : 4 * G] + w[4 * G :]
    w = jnp.where(row < G, w, pltpu.roll(w, TILE - HEAD, 1))
    parts = thirds(w)
    state = jnp.where(lane < HEAD, parts[0], 0.0)
    for i in (1, 2):
        state = jnp.where((lane >= i * HEAD) & (lane < (i + 1) * HEAD), pltpu.roll(parts[i], i * HEAD, 1), state)
    for i, column in enumerate((*thirds(total), *thirds(top))):
        state = jnp.where(lane == 96 + i, column, state)
    state_ref[...] = state.astype(BF16)


def masks_kernel(links_ref, map_ref, *refs):
    packs, (bias_ref, w_out_ref, owner_ref) = refs[:REP], refs[REP:]
    owners = map_ref[...] // 16
    for plane in range(REP):
        first = (plane + REP - lax.axis_index("rep")) % REP * 16
        for j in range(16):
            column = 4 * plane + j // 4
            owner = owners[j % 4 : j % 4 + 1, column : column + 1]
            owner_ref[first + j] = jnp.broadcast_to(owner, (1, TILE))
    w_out = jnp.concatenate([p[2 * WIDTH : 3 * WIDTH, :] for p in packs], axis=0)
    w_out_ref[...] = w_out.astype(jnp.float32).T.astype(BF16)
    position = lax.broadcasted_iota(jnp.int32, (TILE, TILE), 0)
    for c in range(4):
        first = pl.multiple_of(lax.axis_index("rep") * 512 + c * TILE, TILE)
        links = links_ref[:, pl.ds(first, TILE)]
        linked = position == links[0:1, :]
        for n in range(1, 16):
            linked = linked | (position == links[n : n + 1, :])
        bias_ref[:, c * TILE : (c + 1) * TILE] = jnp.where(linked, 0.0, NEG)


def project_here_kernel(feat_ref, vs_ref, *refs):
    ns, packs, (key_ref, value_ref) = refs[:2], refs[2 : 2 + REP], refs[2 + REP :]
    w_value = jnp.concatenate([p[:WIDTH, :] for p in packs], axis=0)
    w_key = jnp.concatenate([p[WIDTH : 2 * WIDTH, :] for p in packs], axis=0)
    for c in range(4):
        first = pl.multiple_of(lax.axis_index("rep") * 512 + c * TILE, TILE)
        here = [feat_ref[pl.ds(first, TILE), :], ns[c // 2][c % 2 * 4 : c % 2 * 4 + 4].reshape(TILE, D)]
        key_ref[c] = dot(jnp.concatenate([*here, vs_ref[:16, :]], axis=0), w_key, NT).astype(BF16)
        value_ref[c] = dot(w_value, jnp.concatenate([*here, vs_ref[...]], axis=0), NT).astype(BF16)


def attention(blocks, feat_ref, ns, bias_ref, packs, here_refs, w_out_ref, key_ref, value_ref, score_ref, weight_ref, query_ref):
    lane = lax.broadcasted_iota(jnp.int32, (TILE, TILE), 1)
    row = lax.broadcasted_iota(jnp.int32, (16, 2 * TILE), 0)
    w_value = jnp.concatenate([p[:WIDTH, :] for p in packs], axis=0)
    w_key = jnp.concatenate([p[WIDTH : 2 * WIDTH, :] for p in packs], axis=0)
    w_query = jnp.concatenate([p[3 * WIDTH :, :] for p in packs], axis=0)
    for b in range(2):
        weight_ref[b, HERE : 3 * TILE, :] = jnp.zeros((3 * TILE - HERE, 2 * TILE), BF16)

    def project(i):
        first = pl.multiple_of(lax.axis_index("rep") * 512 + blocks[i] * TILE, TILE)
        own = feat_ref[pl.ds(first, TILE), :]
        near = jnp.concatenate([n[4 * i : 4 * i + 4].reshape(TILE, D) for n in ns], axis=0)
        key_ref[i] = dot(near, w_key, NT).astype(BF16)
        q = dot(own, w_query, NT)
        for pair in range(4):
            part = q[:, pair // 2 * TILE : (pair // 2 + 1) * TILE]
            for k in range(2):
                low = (2 * pair + k) % 4 * HEAD
                masked = jnp.where((lane >= low) & (lane < low + HEAD), part, 0.0).astype(BF16)
                query_ref[i, pair, k * TILE : (k + 1) * TILE, :] = masked

    def project_values(i):
        near = jnp.concatenate([n[4 * i : 4 * i + 4].reshape(TILE, D) for n in ns], axis=0)
        value_ref[i] = dot(w_value, near, NT).astype(BF16)

    def score(n):
        i, pair = divmod(n, 4)
        part = slice(pair // 2 * TILE, (pair // 2 + 1) * TILE)
        here = dot(here_refs[0][blocks[i], :, part], query_ref[i, pair], NT)
        near = dot(key_ref[i, :, part], query_ref[i, pair], NT)
        bias = bias_ref[:, blocks[i] * TILE : (blocks[i] + 1) * TILE]
        bias = jnp.concatenate([bias, bias], axis=1)
        virtual = jnp.where(row < G, here[2 * TILE :], NEG)
        score_ref[n % 2] = jnp.concatenate([here[:TILE] + bias, here[TILE : 2 * TILE], virtual, near], axis=0)

    def weigh(n):
        s = score_ref[n % 2]
        p = jnp.exp2((s - jnp.max(s, axis=0, keepdims=True)) * EXP2_SCALE)
        weight_ref[n % 2, :HERE, :] = p[:HERE].astype(BF16)
        weight_ref[n % 2, 3 * TILE :, :] = p[HERE:].astype(BF16)
        return 1.0 / jnp.sum(p, axis=0, keepdims=True)

    def blend(n, scale):
        i, pair = divmod(n, 4)
        rows = slice(pair * WIDTH, (pair + 1) * WIDTH)
        values = jnp.concatenate([here_refs[1][blocks[i], rows, :], value_ref[i, rows, :]], axis=1)
        o = dot(values, weight_ref[n % 2]) * scale
        return jnp.concatenate([o[:HEAD, :TILE], o[HEAD:, TILE:]], axis=0)

    project(0)
    score(0)
    parts, scale = [], None
    for n in range(4 * len(blocks)):
        if n + 1 < 4 * len(blocks):
            score(n + 1)
        if n % 4 == 0:
            project_values(n // 4)
        if n % 4 == 1 and n // 4 + 1 < len(blocks):
            project(n // 4 + 1)
        if n:
            parts.append(blend(n - 1, scale))
        scale = weigh(n)
    parts.append(blend(4 * len(blocks) - 1, scale))
    heads = [jnp.concatenate(parts[4 * i : 4 * i + 4], axis=0) for i in range(len(blocks))]
    return dot(w_out_ref[...], jnp.concatenate(heads, axis=1).astype(BF16)).astype(BF16)


def attention_kernel(chunk, feat_ref, *refs):
    ns, refs = refs[: REP - 1], refs[REP - 1 :]
    bias_ref, refs = refs[0], refs[1:]
    packs, refs = refs[:REP], refs[REP:]
    here_refs, w_out_ref, refs = refs[:2], refs[2], refs[3:]
    refs, scratch = refs[:-5], refs[-5:]
    out = attention(CHUNKS[chunk], feat_ref, ns, bias_ref, packs, here_refs, w_out_ref, *scratch)
    if chunk == 0:
        refs[0][...] = out
        return
    heads_ref, before_ref, *outs, own_ref = refs
    own_ref[...] = out
    done = before_ref.shape[1]
    for d in range(REP):
        first = pl.multiple_of(((lax.axis_index("rep") + d) % REP) * WIDTH, WIDTH)
        outs[d][:WIDTH, :done] = before_ref[pl.ds(first, WIDTH), :]
        outs[d][:WIDTH, done:] = own_ref[pl.ds(first, WIDTH), :]
        outs[d][WIDTH:, :TILE] = heads_ref[...]
        outs[d][WIDTH:, TILE:] = jnp.zeros((2 * G, 3 * TILE), BF16)


def assemble_kernel(*refs):
    pieces, packs, (out_ref, virtual_ref, scratch) = refs[:REP], refs[REP : 2 * REP], refs[2 * REP :]
    total = jnp.zeros((2 * G, D), jnp.float32)
    for d in range(REP):
        first = pl.multiple_of(((lax.axis_index("rep") + REP - d) % REP) * 512, 512)
        out_ref[:, pl.ds(first, 512)] = pieces[d][:WIDTH, :]
        total = total + dot(pieces[d][WIDTH:, :TILE], packs[d][TILE:, :])
    scratch[...] = total.T
    own = scratch[pl.ds(pl.multiple_of(lax.axis_index("rep") * WIDTH, WIDTH), WIDTH), :]
    virtual_ref[...] = own.T[:G, :].astype(BF16)


def send_rep(values):
    received = list(values)
    for d in (1, 3, 2):
        received[d] = lax.ppermute(values[d], "rep", [(i, (i + d) % REP) for i in range(REP)])
    return received


def shards(features, virtual_state, w_query, w_key, w_value, w_out, tile_map, local_nbr):
    map_t = tile_map.T

    wanted_from = pl.pallas_call(
        wanted_rows_kernel,
        out_shape=vmem_out((PEERS, TILE), jnp.int32),
        in_specs=[VMEM],
        out_specs=VMEM,
        compiler_params=params(2),
        name="wanted_rows",
    )(in_vmem(map_t))
    wanted = lax.all_to_all(wanted_from.reshape(PEERS, 1, TILE), "nodes", 0, 0, tiled=True)

    rows_in_vmem, pack, virtual_rows, state = pl.pallas_call(
        prepare_kernel,
        out_shape=[
            vmem_out((2048, D), BF16),
            vmem_out((D, D), BF16),
            vmem_out((TILE, D), BF16),
            vmem_out((2 * G, TILE), BF16),
        ],
        in_specs=[pl.BlockSpec(memory_space=pl.ANY)] * 5 + [VMEM],
        out_specs=[VMEM] * 4,
        scratch_shapes=[pltpu.SemaphoreType.DMA((4 + PIECES,))],
        compiler_params=params(16),
        name="prepare",
    )(*map(in_hbm, (features, w_value.T, w_key.T, w_out, w_query.T)), virtual_state)
    packs = [in_vmem(p) for p in send_rep([pack] * REP)]

    bias, w_out_t, owners = pl.pallas_call(
        masks_kernel,
        out_shape=[
            vmem_out((TILE, 512), jnp.float32),
            vmem_out((D, D), BF16),
            vmem_out((PEERS, 1, TILE), jnp.int32),
        ],
        in_specs=[VMEM] * (2 + REP),
        out_specs=[VMEM] * 3,
        compiler_params=params(2),
        name="masks",
    )(local_nbr.T, map_t, *packs)

    outgoing = pl.pallas_call(
        gather_send_kernel,
        out_shape=jax.ShapeDtypeStruct((PEERS, 8, 9 * TILE), BF16),
        in_specs=[VMEM] * 3,
        out_specs=pl.BlockSpec(memory_space=pl.ANY),
        scratch_shapes=[pltpu.VMEM((PEERS, 8, 9 * TILE), BF16), pltpu.SemaphoreType.DMA((PIECES,))],
        compiler_params=params(4),
        name="gather_send",
    )(in_vmem(wanted.reshape(PEERS, TILE)), in_vmem(rows_in_vmem.reshape(PEERS, QUARTER, D)), in_vmem(state))
    arrived = lax.all_to_all(outgoing, "nodes", 0, 0, tiled=True)

    pieces = []
    for blocks in CHUNKS:
        sends = pl.pallas_call(
            lambda *refs, blocks=blocks: gather_rep_kernel(blocks, *refs),
            out_shape=[vmem_out((4 * len(blocks), QUARTER, D), BF16)] * REP,
            in_specs=[VMEM] * 2,
            out_specs=[VMEM] * REP,
            compiler_params=params(2),
        )(in_vmem(owners), in_vmem(arrived))
        pieces.append(send_rep(sends))
    heads = pl.pallas_call(
        join_virtual_kernel,
        out_shape=vmem_out((2 * G, TILE), BF16),
        in_specs=[VMEM],
        out_specs=VMEM,
        compiler_params=params(4),
        name="join_virtual",
    )(in_vmem(arrived))

    here = pl.pallas_call(
        project_here_kernel,
        out_shape=[vmem_out((4, HERE, D), BF16), vmem_out((4, D, 3 * TILE), BF16)],
        in_specs=[VMEM] * (4 + REP),
        out_specs=[VMEM] * 2,
        compiler_params=params(4),
        name="project_here",
    )(*map(in_vmem, (rows_in_vmem, virtual_rows, pieces[0][0], pieces[1][0])), *packs)

    rows = None
    for k, blocks in enumerate(CHUNKS):
        last = k == len(CHUNKS) - 1
        args = [in_vmem(rows_in_vmem), *map(in_vmem, pieces[k][1:]), in_vmem(bias), *packs]
        args += map(in_vmem, (*here, w_out_t))
        args += [in_vmem(heads), in_vmem(rows)] if last else []
        count = len(blocks)
        rows = pl.pallas_call(
            lambda *refs, k=k: attention_kernel(k, *refs),
            out_shape=[vmem_out((WIDTH + 2 * G, 512), BF16)] * REP if last else vmem_out((D, count * TILE), BF16),
            in_specs=[VMEM] * len(args),
            out_specs=[VMEM] * REP if last else VMEM,
            scratch_shapes=[pltpu.VMEM((D, count * TILE), BF16)] * last
            + [
                pltpu.VMEM((count, 3 * TILE, D), BF16),
                pltpu.VMEM((count, D, 3 * TILE), BF16),
                pltpu.VMEM((2, KEYS, 2 * TILE), jnp.float32),
                pltpu.VMEM((2, 6 * TILE, 2 * TILE), BF16),
                pltpu.VMEM((count, 4, 2 * TILE, TILE), BF16),
            ],
            compiler_params=pltpu.CompilerParams(vmem_limit_bytes=24 * 1024 * 1024),
        )(*args)
    received = send_rep(rows)
    return_shape = [jax.ShapeDtypeStruct((WIDTH, 2048), BF16), jax.ShapeDtypeStruct((G, WIDTH), BF16)]
    node_out, virtual_out = pl.pallas_call(
        assemble_kernel,
        out_shape=return_shape,
        in_specs=[VMEM] * (2 * REP),
        out_specs=[VMEM] * 2,
        scratch_shapes=[pltpu.VMEM((D, 2 * G), jnp.float32)],
        compiler_params=params(4),
        name="assemble",
    )(*map(in_vmem, received), *packs)
    return node_out.T, virtual_out


def solution(mesh):
    in_specs = (
        P("nodes", None),
        P(),
        P(None, "rep"),
        P(None, "rep"),
        P(None, "rep"),
        P("rep", None),
        P("nodes", None),
        P("nodes", None),
    )
    out_specs = (P("nodes", "rep"), P(None, "rep"))
    return jax.shard_map(shards, mesh=mesh, in_specs=in_specs, out_specs=out_specs, check_vma=False)
```
